32 devices in a mesh: dp: 2 (over x), tp: 4 (over z), pp: 4 (over y, core).
Axes of the slice: x: 2, y: 2, z: 4, core: 2. Of those that a mesh axis runs over, the one named last changes fastest.
Arguments:
- tok_ids: int32 [8, 1, 512], P(('dp', 'pp')), parts along dimension 0
- hid_in: bfloat16 [8, 1, 512, 128], P(('dp', 'pp')), parts along dimension 0
- cot_in: bfloat16 [8, 1, 512, 128], P(('dp', 'pp')), parts along dimension 0
- ln_gamma: float32 [8, 128], P(('dp', 'pp')), parts along dimension 0
- ln_beta: float32 [8, 128], P(('dp', 'pp')), parts along dimension 0
- emb_table: bfloat16 [8, 50304, 128], P(('dp', 'pp'), 'tp'), parts along dimension 0
- w_in: bfloat16 [8, 128, 512], P(('dp', 'pp'), None, 'tp'), parts along dimension 0
- b_in: float32 [8, 512], P(('dp', 'pp'), 'tp'), parts along dimension 0
- w_out: bfloat16 [8, 512, 128], P(('dp', 'pp'), 'tp'), parts along dimension 0
Outputs:
- output 1: float32 [8, 50304, 128], P(('dp', 'pp'), 'tp'), parts along dimension 0
- output 2: float32 [8], P(('dp', 'pp')), parts along dimension 0
- output 3: float32 [8, 128], P(('dp', 'pp')), parts along dimension 0
- output 4: float32 [8, 128], P(('dp', 'pp')), parts along dimension 0
- output 5: float32 [8, 128, 512], P(('dp', 'pp'), None, 'tp'), parts along dimension 0
- output 6: float32 [8, 512], P(('dp', 'pp'), 'tp'), parts along dimension 0
- output 7: float32 [8, 512, 128], P(('dp', 'pp'), 'tp'), parts along dimension 0
There are 2 independent parts. The reference program is written for one: setup_inputs(seed, part) draws one part's arguments, and reference() takes and returns one part's arrays. A program takes and returns all parts, laid end to end along the dimension named above; each array names one.
All inputs are finite; a program needn't handle non-finite values.
Results may differ from the reference program's by a relative error of at most 0.00333534.
Values sent between devices are 32-bit elements.
A program may use at most 1 GiB of HBM per device.

```python
import jax
import jax.numpy as jnp
from jax import lax

STAGES = 4
NUM_SEQS = 1
SEQ_LEN = 512
D_MODEL = 128
VOCAB_SIZE = 50304
HOT_IDS = 64
FF_DIM = 4 * D_MODEL
LN_EPS = 1e-5


def draw_ids(key_ids, key_hot):
    shape_ids = (STAGES, NUM_SEQS, SEQ_LEN)
    hot_list = jax.random.randint(key_hot, (HOT_IDS,), 0, VOCAB_SIZE)
    key_pick, key_unif, key_coin = jax.random.split(key_ids, 3)
    picked = hot_list[jax.random.randint(key_pick, shape_ids, 0, HOT_IDS)]
    uniform_ids = jax.random.randint(key_unif, shape_ids, 0, VOCAB_SIZE)
    coin_flip = jax.random.randint(key_coin, shape_ids, 0, 2)
    drawn_ids = jnp.where(coin_flip == 0, picked, uniform_ids)
    drawn_ids = drawn_ids.at[:, 0, 0].set(0).at[:, 0, 1].set(VOCAB_SIZE - 1)
    return drawn_ids.astype(jnp.int32)


def setup_inputs(seed: int = 0, part: int = 0) -> dict:
    part_key = jax.random.fold_in(jax.random.key(seed), part)
    key_list = jax.random.split(part_key, 10)
    act_shape = (STAGES, NUM_SEQS, SEQ_LEN, D_MODEL)
    tok_ids = draw_ids(key_list[0], key_list[1])
    hid_in = jax.random.normal(key_list[2], act_shape, jnp.float32).astype(jnp.bfloat16)
    cot_in = (jax.random.normal(key_list[3], act_shape, jnp.float32) * 3.5 * D_MODEL ** -0.5).astype(jnp.bfloat16)
    ln_gamma = 1.0 + 0.3 * jax.random.normal(key_list[4], (STAGES, D_MODEL), jnp.float32)
    ln_beta = 0.3 * jax.random.normal(key_list[5], (STAGES, D_MODEL), jnp.float32)
    one_table = jax.random.normal(key_list[6], (VOCAB_SIZE, D_MODEL), jnp.float32) * 3.5 * D_MODEL ** -0.5
    emb_table = jnp.broadcast_to(one_table.astype(jnp.bfloat16)[None], (STAGES, VOCAB_SIZE, D_MODEL))
    w_in = (jax.random.normal(key_list[7], (STAGES, D_MODEL, FF_DIM), jnp.float32) * D_MODEL ** -0.5).astype(jnp.bfloat16)
    b_in = 0.5 * jax.random.normal(key_list[8], (STAGES, FF_DIM), jnp.float32)
    w_out = (jax.random.normal(key_list[9], (STAGES, FF_DIM, D_MODEL), jnp.float32) * FF_DIM ** -0.5).astype(jnp.bfloat16)
    return {'tok_ids': tok_ids, 'hid_in': hid_in, 'cot_in': cot_in, 'ln_gamma': ln_gamma, 'ln_beta': ln_beta, 'emb_table': emb_table, 'w_in': w_in, 'b_in': b_in, 'w_out': w_out}


def ln_apply(rows_f, ln_gain, ln_shift):
    centre = rows_f - jnp.mean(rows_f, axis=-1, keepdims=True)
    inv_std = lax.rsqrt(jnp.mean(centre * centre, axis=-1, keepdims=True) + LN_EPS)
    return centre * inv_std * ln_gain + ln_shift


def gelu_tanh(values):
    return jax.nn.gelu(values, approximate=True)


def first_stage(tok_flat, cot_rows, ln_gain, ln_shift, vocab_tab):
    emb_rows = vocab_tab[tok_flat].astype(jnp.float32)
    pull_back = jax.vjp(ln_apply, emb_rows, ln_gain, ln_shift)[1]
    ln_grads = pull_back(cot_rows.astype(jnp.float32))
    d_rows = ln_grads[0].astype(jnp.bfloat16).astype(jnp.float32)
    first_grad = jax.ops.segment_sum(d_rows, tok_flat, num_segments=VOCAB_SIZE)
    return first_grad, ln_grads[1], ln_grads[2]


def last_stage(label_ids, hid_rows, ln_gain, ln_shift, vocab_tab):
    vocab_pos = jnp.arange(VOCAB_SIZE)

    def seq_step(scan_carry, seq_in):
        grad_acc, gain_acc, shift_acc, loss_acc = scan_carry
        labels_seq, hid_seq = seq_in
        normed, pull_back = jax.vjp(ln_apply, hid_seq.astype(jnp.float32), ln_gain, ln_shift)
        normed_b = normed.astype(jnp.bfloat16)
        logits = jnp.dot(normed_b, vocab_tab.T, preferred_element_type=jnp.float32)
        top_val = jnp.max(logits, axis=-1, keepdims=True)
        exp_vals = jnp.exp(logits - top_val)
        sum_exp = jnp.sum(exp_vals, axis=-1, keepdims=True)
        label_hit = vocab_pos[None, :] == labels_seq[:, None]
        target = jnp.sum(jnp.where(label_hit, logits, 0.0), axis=-1)
        token_loss = jnp.log(sum_exp[:, 0]) + top_val[:, 0] - target
        grad_logits = (exp_vals / sum_exp - label_hit.astype(jnp.float32)).astype(jnp.bfloat16)
        grad_acc = grad_acc + jnp.dot(grad_logits.T, normed_b, preferred_element_type=jnp.float32)
        d_normed = jnp.dot(grad_logits, vocab_tab, preferred_element_type=jnp.float32)
        ln_grads = pull_back(d_normed)
        new_carry = (grad_acc, gain_acc + ln_grads[1], shift_acc + ln_grads[2], loss_acc + jnp.sum(token_loss))
        return new_carry, None

    init_carry = (jnp.zeros((VOCAB_SIZE, D_MODEL), jnp.float32), jnp.zeros((D_MODEL,), jnp.float32), jnp.zeros((D_MODEL,), jnp.float32), jnp.zeros((), jnp.float32))
    final_carry = lax.scan(seq_step, init_carry, (label_ids, hid_rows))[0]
    return final_carry[0], final_carry[1], final_carry[2], final_carry[3] / (NUM_SEQS * SEQ_LEN)


def middle_stage(stage_in):
    hid_rows, cot_rows, ln_gain, ln_shift, w_first, bias_first, w_second = stage_in
    rows_f = hid_rows.reshape(-1, D_MODEL).astype(jnp.float32)
    cot_b = cot_rows.reshape(-1, D_MODEL)
    normed, pull_back = jax.vjp(ln_apply, rows_f, ln_gain, ln_shift)
    normed_b = normed.astype(jnp.bfloat16)
    pre_act = jnp.dot(normed_b, w_first, preferred_element_type=jnp.float32) + bias_first
    act_val, gelu_back = jax.vjp(gelu_tanh, pre_act)
    w2_grad = jnp.dot(act_val.astype(jnp.bfloat16).T, cot_b, preferred_element_type=jnp.float32)
    d_act = jnp.dot(cot_b, w_second.T, preferred_element_type=jnp.float32)
    d_pre = gelu_back(d_act)[0]
    d_pre_b = d_pre.astype(jnp.bfloat16)
    w1_grad = jnp.dot(normed_b.T, d_pre_b, preferred_element_type=jnp.float32)
    b1_grad = jnp.sum(d_pre, axis=0)
    d_normed = jnp.dot(d_pre_b, w_first.T, preferred_element_type=jnp.float32)
    ln_grads = pull_back(d_normed)
    return ln_grads[1], ln_grads[2], w1_grad, b1_grad, w2_grad


def reference(tok_ids, hid_in, cot_in, ln_gamma, ln_beta, emb_table, w_in, b_in, w_out):
    last_slot = STAGES - 1
    first_grad, first_gain, first_shift = first_stage(tok_ids[0].reshape(-1), cot_in[0].reshape(-1, D_MODEL), ln_gamma[0], ln_beta[0], emb_table[0])
    last_grad, last_gain, last_shift, loss_val = last_stage(tok_ids[last_slot], hid_in[last_slot], ln_gamma[last_slot], ln_beta[last_slot], emb_table[last_slot])
    tied_grad = first_grad + last_grad
    mid_in = (hid_in[1:last_slot], cot_in[1:last_slot], ln_gamma[1:last_slot], ln_beta[1:last_slot], w_in[1:last_slot], b_in[1:last_slot], w_out[1:last_slot])
    mid_gain, mid_shift, mid_w1, mid_b1, mid_w2 = lax.map(middle_stage, mid_in)
    zero_tab = jnp.zeros((STAGES - 2, VOCAB_SIZE, D_MODEL), jnp.float32)
    emb_grad = jnp.concatenate([tied_grad[None], zero_tab, tied_grad[None]], axis=0)
    loss_out = jnp.concatenate([jnp.zeros((last_slot,), jnp.float32), loss_val[None]])
    gamma_grad = jnp.concatenate([first_gain[None], mid_gain, last_gain[None]], axis=0)
    beta_grad = jnp.concatenate([first_shift[None], mid_shift, last_shift[None]], axis=0)
    zero_w1 = jnp.zeros((1, D_MODEL, FF_DIM), jnp.float32)
    zero_b1 = jnp.zeros((1, FF_DIM), jnp.float32)
    zero_w2 = jnp.zeros((1, FF_DIM, D_MODEL), jnp.float32)
    w_in_grad = jnp.concatenate([zero_w1, mid_w1, zero_w1], axis=0)
    b_in_grad = jnp.concatenate([zero_b1, mid_b1, zero_b1], axis=0)
    w_out_grad = jnp.concatenate([zero_w2, mid_w2, zero_w2], axis=0)
    return emb_grad, loss_out, gamma_grad, beta_grad, w_in_grad, b_in_grad, w_out_grad
```

```python
import functools

import jax
import jax.numpy as jnp
from jax import lax
from jax.experimental import pallas as pl
from jax.experimental.pallas import tpu as pltpu
from jax.sharding import PartitionSpec as P

F = jnp.float32
B = jnp.bfloat16
LN_EPS = 1e-5
LOG2E = 1.4426950408889634
LANES = 128
TILE = 256
MESH = pl.DeviceIdType.MESH
NT = (((1,), (1,)), ((), ()))
TN = (((0,), (0,)), ((), ()))


def ln_hat(rows):
    centre = rows - jnp.mean(rows, axis=-1, keepdims=True)
    inv = lax.rsqrt(jnp.mean(centre * centre, axis=-1, keepdims=True) + LN_EPS)
    return centre * inv, inv


def mm(a, b):
    return jnp.dot(a, b, preferred_element_type=F)


def lanes_row(ref, first, chunks):
    return jnp.concatenate([ref[first + c:first + c + 1, :] for c in range(chunks)], axis=1)


def stats_kernel(cfg, ids_ref, hid_ref, cot_ref, gam_ref, bet_ref, emb_hbm,
                 y_out, lab_out, lse_out, dx_out, did_out, xh_out, part_out,
                 e_ref, yt_ref, buf, pack_src, pack_dst, dx_src, dx_dst, st_src, st_all, xt_ref,
                 e_sem, send_sem, pack_sem, dx_sem, st_sem):
    stages, tps, toks, dim, vocab = cfg
    chunks = toks // LANES
    rank = lax.axis_index('tp')
    stage = lax.axis_index('pp')
    last = stages - 1
    helper = stages - 2
    e_copy = pltpu.make_async_copy(emb_hbm, e_ref, e_sem)
    full, tail = vocab // TILE - 1, vocab - (vocab // TILE - 1) * TILE

    def pack_copy(to_stage, idx):
        return pltpu.make_async_remote_copy(pack_src, pack_dst, send_sem.at[idx], pack_sem, device_id={'pp': to_stage, 'tp': rank}, device_id_type=MESH)

    def dx_copy():
        return pltpu.make_async_remote_copy(dx_src, dx_dst, send_sem.at[0], dx_sem, device_id={'pp': last, 'tp': rank}, device_id_type=MESH)

    def st_copy(to_stage, off, idx):
        return pltpu.make_async_remote_copy(st_src, st_all.at[rank], send_sem.at[idx], st_sem.at[rank], device_id={'pp': to_stage, 'tp': lax.rem(rank + off, tps)}, device_id_type=MESH)

    def signal_to(to_stage, offs):
        bar = pltpu.get_barrier_semaphore()
        for off in offs:
            pl.semaphore_signal(bar, inc=1, device_id={'pp': to_stage, 'tp': lax.rem(rank + off, tps)}, device_id_type=MESH)

    def normed(rows, gam, bet):
        hat, _ = ln_hat(rows)
        return hat, (hat * gam + bet).astype(B)

    def finish_stats():
        tops = [st_all[r, 0:chunks, :] for r in range(tps)]
        sums = [st_all[r, chunks:2 * chunks, :] for r in range(tps)]
        top = functools.reduce(jnp.maximum, tops)
        tot = functools.reduce(jnp.add, [s * jnp.exp(t - top) for s, t in zip(sums, tops)])
        lse_out[0:chunks, :] = top + jnp.log(tot)

    def unpack():
        hat, norm = normed(pack_dst[0:toks, :], pack_dst[toks + chunks:toks + chunks + 1, :], pack_dst[toks + chunks + 1:toks + chunks + 2, :])
        xh_out[...] = hat
        y_out[...] = norm
        lab_out[0:chunks, :] = pack_dst[toks:toks + chunks, :].astype(jnp.int32)

    @pl.when(stage == last)
    def _():
        e_copy.start()
        signal_to(0, range(tps))
        signal_to(helper, range(tps))
        signal_to(last, range(1, tps))
        rows = hid_ref[...].astype(F)
        pack_src[0:toks, :] = rows
        pack_src[toks:toks + chunks, :] = ids_ref[...].astype(F)
        pack_src[toks + chunks:toks + chunks + 1, :] = gam_ref[...]
        pack_src[toks + chunks + 1:toks + chunks + 2, :] = bet_ref[...]
        hat, norm = normed(rows, gam_ref[...], bet_ref[...])
        xh_out[...] = hat
        y_out[...] = norm
        lab_out[0:chunks, :] = ids_ref[...]
        yt_ref[...] = norm.astype(F).T.astype(B)
        pl.semaphore_wait(pltpu.get_barrier_semaphore(), 3 * tps - 1)
        pack_copy(0, 0).start()
        pack_copy(helper, 1).start()
        e_copy.wait()

        def logits_to(row, slot, top):
            logits = mm(e_ref[pl.ds(row, TILE), :], yt_ref[...])
            buf[slot] = logits
            return jnp.maximum(top, jnp.max(logits.reshape(TILE // 8, 8, toks), axis=0))

        def add_exp(slot, top_old, top, tot):
            ex = jnp.exp(buf[slot].reshape(TILE // 8, 8, toks) - top[None])
            return tot * jnp.exp(top_old - top) + jnp.sum(ex, axis=0)

        top0 = jnp.full((8, toks), -jnp.inf, F)
        top1 = logits_to(0, 0, top0)
        top0 = top1
        tot = jnp.zeros((8, toks), F)

        def step(i, carry):
            old, top, tot = carry
            row = pl.multiple_of(i * 2 * TILE, TILE)
            mid = logits_to(row + TILE, 1, top)
            tot = add_exp(0, old, top, tot)
            new = logits_to(row + 2 * TILE, 0, mid)
            tot = add_exp(1, top, mid, tot)
            return mid, new, tot

        pairs = (full - 2) // 2
        old, top, tot = lax.fori_loop(0, pairs, step, (top0, top1, tot), unroll=4)
        mid = logits_to((2 * pairs + 1) * TILE, 1, top)
        tot = add_exp(0, old, top, tot)
        tot = add_exp(1, top, mid, tot)
        logits = mm(e_ref[full * TILE:vocab, :], yt_ref[...]).reshape(tail // 8, 8, toks)
        new = jnp.maximum(mid, jnp.max(logits, axis=0))
        tot = tot * jnp.exp(mid - new) + jnp.sum(jnp.exp(logits - new[None]), axis=0)
        top = jnp.max(new, axis=0, keepdims=True)
        tot = jnp.sum(tot * jnp.exp(new - top), axis=0, keepdims=True)
        for c in range(chunks):
            st_src[c:c + 1, :] = top[:, c * LANES:(c + 1) * LANES]
            st_src[chunks + c:chunks + c + 1, :] = tot[:, c * LANES:(c + 1) * LANES]
        st_all[rank] = st_src[...]
        copies = []
        for to_stage, offs in ((last, range(1, tps)), (0, range(tps)), (helper, range(tps))):
            for off in offs:
                copies.append(st_copy(to_stage, off, 2 + len(copies)))
        for copy in copies:
            copy.start()
        for off in range(1, tps):
            src = lax.rem(rank + off, tps)
            pltpu.make_async_remote_copy(st_src, st_all.at[src], send_sem.at[0], st_sem.at[src], device_id={'pp': last, 'tp': rank}, device_id_type=MESH).wait_recv()
        finish_stats()
        dx_copy().wait_recv()
        dx_out[...] = dx_dst[0:toks, :].astype(B)
        did_out[0:chunks, :] = dx_dst[toks:toks + chunks, :].astype(jnp.int32)
        pack_copy(0, 0).wait_send()
        pack_copy(helper, 1).wait_send()
        for copy in copies:
            copy.wait_send()

    @pl.when(stage == 0)
    def _():
        e_copy.start()
        signal_to(last, range(tps))
        e_copy.wait()
        local = lanes_row(ids_ref, 0, chunks) - rank * vocab
        xt_ref[...] = jnp.zeros((dim, toks), F)

        def pick(row, size):
            rows = lax.broadcasted_iota(jnp.int32, (size, toks), 0) + row
            hit = jnp.where(rows == local, 1.0, 0.0).astype(B)
            xt_ref[...] += lax.dot_general(e_ref[pl.ds(row, size), :], hit, TN, preferred_element_type=F)

        def step(i, carry):
            pick(pl.multiple_of(i * TILE, TILE), TILE)
            return carry

        lax.fori_loop(0, full, step, 0, unroll=4)
        pick(full * TILE, tail)
        inside = jnp.where((local >= 0) & (local < vocab), 1.0, 0.0)
        mask = jnp.broadcast_to(inside, (LANES, toks)).T
        hat, inv = ln_hat(xt_ref[...].T)
        cot = cot_ref[...].astype(F)
        scaled = cot * gam_ref[...]
        grad = inv * (scaled - jnp.mean(scaled, axis=-1, keepdims=True) - hat * jnp.mean(scaled * hat, axis=-1, keepdims=True))
        grad = jnp.where(mask > 0.5, grad, 0.0).astype(B)
        dx_out[...] = grad
        did_out[0:chunks, :] = ids_ref[...]
        dx_src[0:toks, :] = grad.astype(F)
        dx_src[toks:toks + chunks, :] = ids_ref[...].astype(F)
        part_out[0:1, :] = jnp.sum(jnp.where(mask > 0.5, cot * hat, 0.0), axis=0, keepdims=True)
        part_out[1:2, :] = jnp.sum(jnp.where(mask > 0.5, cot, 0.0), axis=0, keepdims=True)
        pl.semaphore_wait(pltpu.get_barrier_semaphore(), tps)
        dx_copy().start()
        pack_copy(0, 0).wait_recv()
        unpack()
        for r in range(tps):
            pltpu.make_async_remote_copy(st_src, st_all.at[r], send_sem.at[0], st_sem.at[r], device_id={'pp': last, 'tp': rank}, device_id_type=MESH).wait_recv()
        finish_stats()
        dx_copy().wait_send()

    @pl.when(stage == helper)
    def _():
        signal_to(last, range(tps))
        pl.semaphore_wait(pltpu.get_barrier_semaphore(), tps)
        pack_copy(0, 0).wait_recv()
        unpack()
        for r in range(tps):
            pltpu.make_async_remote_copy(st_src, st_all.at[r], send_sem.at[0], st_sem.at[r], device_id={'pp': last, 'tp': rank}, device_id_type=MESH).wait_recv()
        finish_stats()


def grad_kernel(cfg, emb_hbm, y_ref, lab_ref, lse_ref, dx_ref, did_ref, xh_ref, pin_ref,
                hid_ref, cot_ref, gam_ref, bet_ref, w1_ref, b1_ref, w2_ref,
                emb_out, w1_out, b1_out, w2_out, part_out,
                e_ref, ya_ref, out_ref, dyt_ref, e_sem, o_sem):
    stages, tps, toks, dim, vocab = cfg
    chunks = toks // LANES
    rank = lax.axis_index('tp')
    stage = lax.axis_index('pp')
    last = stages - 1
    helper = stages - 2
    base = rank * vocab
    full, tail = vocab // TILE - 1, vocab - (vocab // TILE - 1) * TILE
    group = 8
    groups = full // group
    e_copy = pltpu.make_async_copy(emb_hbm, e_ref, e_sem)

    def out_copy(c):
        size = tail if c == groups else group * TILE
        return pltpu.make_async_copy(out_ref.at[pl.ds(c * group * TILE, size)], emb_out.at[pl.ds(c * group * TILE, size)], o_sem.at[c])

    def prepare():
        ya_ref[0:dim, :] = y_ref[...].astype(F).T.astype(B)
        lse = lanes_row(lse_ref, 0, chunks)
        hi = (lse * 0.99609375).astype(B)
        rest = lse - hi.astype(F)
        mid = rest.astype(B)
        low = (rest - mid.astype(F)).astype(B)
        pick = lax.broadcasted_iota(jnp.int32, (dim, toks), 0)
        zero = jnp.zeros((dim, toks), F)
        add = jnp.where(pick == 0, -hi.astype(F), jnp.where(pick == 1, -mid.astype(F), jnp.where(pick == 2, -low.astype(F), zero)))
        ya_ref[dim:2 * dim, :] = add.astype(B)

    def shifted(row, size):
        rows = jnp.concatenate([e_ref[pl.ds(row, size), :], jnp.ones((size, dim), B)], axis=1)
        return mm(rows, ya_ref[...])

    def zero_parts():
        w1_out[...] = jnp.zeros(w1_out.shape, F)
        b1_out[...] = jnp.zeros(b1_out.shape, F)
        w2_out[...] = jnp.zeros(w2_out.shape, F)

    @pl.when((stage == 0) | (stage == last))
    def _():
        e_copy.start()
        zero_parts()
        part_out[...] = pin_ref[...]
        prepare()
        lab = lanes_row(lab_ref, 0, chunks) - base
        did = lanes_row(did_ref, 0, chunks) - base
        e_copy.wait()

        def work(row, size):
            p = jnp.exp2(shifted(row, size) * LOG2E)
            rows = lax.broadcasted_iota(jnp.int32, (size, LANES), 0) + row
            g, h = [], []
            for c in range(chunks):
                cols = slice(c * LANES, (c + 1) * LANES)
                pc = p[:, cols]
                g.append(jnp.where(rows == lab[:, cols], pc - 1.0, pc).astype(B))
                h.append(jnp.where(rows == did[:, cols], 1.0, 0.0).astype(B))
            out_ref[pl.ds(row, size), :] = mm(jnp.concatenate(g, axis=1), y_ref[...]) + mm(jnp.concatenate(h, axis=1), dx_ref[...])

        for c in range(groups):
            def step(i, carry):
                work(pl.multiple_of(c * group * TILE + i * TILE, TILE), TILE)
                return carry
            lax.fori_loop(0, group, step, 0, unroll=4)
            out_copy(c).start()
        work(full * TILE, tail)
        out_copy(groups).start()
        for c in range(groups + 1):
            out_copy(c).wait()

    @pl.when((stage != 0) & (stage != last))
    def _():
        @pl.when(stage == helper)
        def _():
            e_copy.start()
        size = group * TILE
        out_ref[0:size, :] = jnp.zeros((size, dim), F)

        def zero_copy(c):
            n = tail if c == groups else size
            return pltpu.make_async_copy(out_ref.at[pl.ds(0, n)], emb_out.at[pl.ds(c * size, n)], o_sem.at[c])

        for c in range(groups + 1):
            zero_copy(c).start()
        hat, _ = ln_hat(hid_ref[...].astype(F))
        norm = (hat * gam_ref[...] + bet_ref[...]).astype(B)
        pre = mm(norm, w1_ref[...]) + b1_ref[...]
        cube = 0.7978845608028654 * (pre + 0.044715 * (pre * pre * pre))
        th = jnp.tanh(cube)
        act = pre * (0.5 * (1.0 + th))
        slope = 0.5 * (1.0 + th) + pre * (0.5 * (1.0 - th * th)) * (0.7978845608028654 * (1.0 + 3 * 0.044715 * pre * pre))
        w2_out[...] = lax.dot_general(act.astype(B), cot_ref[...], TN, preferred_element_type=F)
        d_act = lax.dot_general(cot_ref[...], w2_ref[...], NT, preferred_element_type=F)
        d_pre = d_act * slope
        d_b = d_pre.astype(B)
        w1_out[...] = lax.dot_general(norm, d_b, TN, preferred_element_type=F)
        b1_out[...] = jnp.sum(d_pre, axis=0, keepdims=True)
        d_h = lax.dot_general(d_b, w1_ref[...], NT, preferred_element_type=F)
        part_out[0:1, :] = jnp.sum(d_h * hat, axis=0, keepdims=True)
        part_out[1:2, :] = jnp.sum(d_h, axis=0, keepdims=True)

        @pl.when(stage == helper)
        def _():
            prepare()
            lab = lanes_row(lab_ref, 0, chunks) - base
            dyt_ref[...] = jnp.zeros((dim, toks), F)
            e_copy.wait()

            def work(row, size, loss):
                x = shifted(row, size)
                p = jnp.exp2(x * LOG2E)
                rows = lax.broadcasted_iota(jnp.int32, (size, LANES), 0) + row
                g, picked = [], []
                for c in range(chunks):
                    cols = slice(c * LANES, (c + 1) * LANES)
                    hit = rows == lab[:, cols]
                    pc = p[:, cols]
                    g.append(jnp.where(hit, pc - 1.0, pc).astype(B))
                    picked.append(jnp.sum(jnp.where(hit, x[:, cols], 0.0).reshape(size // 8, 8, LANES), axis=0))
                dyt_ref[...] += lax.dot_general(e_ref[pl.ds(row, size), :], jnp.concatenate(g, axis=1), TN, preferred_element_type=F)
                return loss + functools.reduce(jnp.add, picked)

            def step(i, loss):
                return work(pl.multiple_of(i * TILE, TILE), TILE, loss)

            loss = lax.fori_loop(0, full, step, jnp.zeros((8, LANES), F), unroll=4)
            loss = work(full * TILE, tail, loss)
            dy = dyt_ref[...].T
            part_out[2:3, :] = jnp.sum(dy * xh_ref[...], axis=0, keepdims=True)
            part_out[3:4, :] = jnp.sum(dy, axis=0, keepdims=True)
            part_out[4:5, :] = jnp.sum(loss, axis=0, keepdims=True)

        for c in range(groups + 1):
            zero_copy(c).wait()


def sum_kernel(cfg, part_ref, out_ref, got, send_sem, recv_sem):
    stages, tps, toks, dim, vocab = cfg
    rank = lax.axis_index('tp')
    stage = lax.axis_index('pp')
    last = stages - 1
    helper = stages - 2
    bar = pltpu.get_barrier_semaphore()

    def copy_to(to_stage, off, idx):
        return pltpu.make_async_remote_copy(part_ref, got.at[rank], send_sem.at[idx], recv_sem.at[rank], device_id={'pp': to_stage, 'tp': lax.rem(rank + off, tps)}, device_id_type=MESH)

    def arrived(src):
        return pltpu.make_async_remote_copy(part_ref, got.at[src], send_sem.at[0], recv_sem.at[src], device_id={'pp': stage, 'tp': rank}, device_id_type=MESH)

    def greet(to_stage, offs):
        for off in offs:
            pl.semaphore_signal(bar, inc=1, device_id={'pp': to_stage, 'tp': lax.rem(rank + off, tps)}, device_id_type=MESH)

    def total(row):
        return functools.reduce(jnp.add, [got[r, row:row + 1, :] for r in range(tps)])

    @pl.when(stage != last)
    def _():
        greet(stage, range(1, tps))

        @pl.when(stage == helper)
        def _():
            greet(last, range(tps))
            pl.semaphore_wait(bar, 2 * tps - 1)
            for off in range(tps):
                copy_to(last, off, tps + off).start()

        @pl.when(stage != helper)
        def _():
            pl.semaphore_wait(bar, tps - 1)
        for off in range(1, tps):
            copy_to(stage, off, off).start()
        got[rank] = part_ref[...]
        for off in range(1, tps):
            arrived(lax.rem(rank + off, tps)).wait_recv()
        out_ref[0:1, :] = total(0)
        out_ref[1:2, :] = total(1)
        out_ref[2:3, :] = jnp.zeros((1, LANES), F)
        for off in range(1, tps):
            copy_to(stage, off, off).wait_send()

        @pl.when(stage == helper)
        def _():
            for off in range(tps):
                copy_to(last, off, tps + off).wait_send()

    @pl.when(stage == last)
    def _():
        greet(helper, range(tps))
        pl.semaphore_wait(bar, tps)
        for r in range(tps):
            arrived(r).wait_recv()
        out_ref[0:1, :] = total(2)
        out_ref[1:2, :] = total(3)
        loss = jnp.sum(total(4), axis=1, keepdims=True) * (-1.0 / toks)
        out_ref[2:3, :] = jnp.broadcast_to(loss, (1, LANES))


def solution(mesh):
    stages, tps = mesh.shape['pp'], mesh.shape['tp']
    lead = ('dp', 'pp')
    hbm = pl.BlockSpec(memory_space=pl.ANY)
    vmem = pl.BlockSpec(memory_space=pltpu.VMEM)
    S = jax.ShapeDtypeStruct

    def body(tok_ids, hid_in, cot_in, ln_gamma, ln_beta, emb_table, w_in, b_in, w_out):
        dim = hid_in.shape[-1]
        hid = hid_in.reshape(-1, dim)
        cot = cot_in.reshape(-1, dim)
        toks = hid.shape[0]
        ids = tok_ids.reshape(toks // LANES, LANES)
        table = emb_table[0]
        vocab = table.shape[0]
        ff = w_in.shape[2]
        cfg = (stages, tps, toks, dim, vocab)
        rows = toks + 2 * (toks // LANES)
        y, lab, lse, dx, did, xh, part = pl.pallas_call(
            functools.partial(stats_kernel, cfg), name='stats',
            out_shape=(S((toks, dim), B), S((8, LANES), jnp.int32), S((8, LANES), F), S((toks, dim), B), S((8, LANES), jnp.int32), S((toks, dim), F), S((8, LANES), F)),
            in_specs=[vmem] * 5 + [hbm], out_specs=[vmem] * 7,
            scratch_shapes=[
                pltpu.VMEM((vocab, dim), B), pltpu.VMEM((dim, toks), B), pltpu.VMEM((2, TILE, toks), F),
                pltpu.VMEM((rows, dim), F), pltpu.VMEM((rows, dim), F), pltpu.VMEM((rows, dim), F), pltpu.VMEM((rows, dim), F),
                pltpu.VMEM((8, LANES), F), pltpu.VMEM((tps, 8, LANES), F), pltpu.VMEM((dim, toks), F),
                pltpu.SemaphoreType.DMA, pltpu.SemaphoreType.DMA((2 + 3 * tps,)), pltpu.SemaphoreType.DMA, pltpu.SemaphoreType.DMA, pltpu.SemaphoreType.DMA((tps,))],
            compiler_params=pltpu.CompilerParams(collective_id=0, has_side_effects=True, vmem_limit_bytes=40 << 20),
        )(ids, hid, cot, ln_gamma, ln_beta, table)
        groups = (vocab // TILE - 1) // 8 + 1
        emb_grad, w1g, b1g, w2g, part = pl.pallas_call(
            functools.partial(grad_kernel, cfg), name='grads',
            out_shape=(S((vocab, dim), F), S((dim, ff), F), S((1, ff), F), S((ff, dim), F), S((8, LANES), F)),
            in_specs=[hbm] + [vmem] * 14, out_specs=[hbm] + [vmem] * 4,
            scratch_shapes=[
                pltpu.VMEM((vocab, dim), B), pltpu.VMEM((2 * dim, toks), B), pltpu.VMEM((vocab, dim), F), pltpu.VMEM((dim, toks), F),
                pltpu.SemaphoreType.DMA, pltpu.SemaphoreType.DMA((groups,))],
            compiler_params=pltpu.CompilerParams(vmem_limit_bytes=48 << 20),
        )(table, y, lab, lse, dx, did, xh, part, hid, cot, ln_gamma, ln_beta, w_in[0], b_in, w_out[0])
        sums = pl.pallas_call(
            functools.partial(sum_kernel, cfg), name='sums',
            out_shape=S((8, LANES), F), in_specs=[vmem], out_specs=vmem,
            scratch_shapes=[pltpu.VMEM((tps, 8, LANES), F), pltpu.SemaphoreType.DMA((2 * tps,)), pltpu.SemaphoreType.DMA((tps,))],
            compiler_params=pltpu.CompilerParams(collective_id=1, has_side_effects=True),
        )(part)
        return emb_grad[None], sums[2, 0:1], sums[0:1], sums[1:2], w1g[None], b1g, w2g[None]

    specs_in = (P(lead, None, None), P(lead, None, None, None), P(lead, None, None, None), P(lead, None), P(lead, None), P(lead, 'tp', None), P(lead, None, 'tp'), P(lead, 'tp'), P(lead, 'tp', None))
    specs_out = (P(lead, 'tp', None), P(lead), P(lead, None), P(lead, None), P(lead, None, 'tp'), P(lead, 'tp'), P(lead, 'tp', None))
    return jax.shard_map(body, mesh=mesh, in_specs=specs_in, out_specs=specs_out, check_vma=False)
```

```python
import functools

import jax
import jax.numpy as jnp
from jax import lax
from jax.experimental import pallas as pl
from jax.experimental.pallas import tpu as pltpu
from jax.sharding import PartitionSpec as P

F = jnp.float32
B = jnp.bfloat16
LN_EPS = 1e-5
LOG2E = 1.4426950408889634
LANES = 128
TILE = 256
SPLIT_STATS = 34
SPLIT_DY = 26
EARLY = 8
GRANT = 20 << 20
MESH = pl.DeviceIdType.MESH
NT = (((1,), (1,)), ((), ()))
TN = (((0,), (0,)), ((), ()))


def ln_hat(rows):
    centre = rows - jnp.mean(rows, axis=-1, keepdims=True)
    inv = lax.rsqrt(jnp.mean(centre * centre, axis=-1, keepdims=True) + LN_EPS)
    return centre * inv, inv


def mm(a, b):
    return jnp.dot(a, b, preferred_element_type=F)


def lanes_row(ref, first, chunks):
    return jnp.concatenate([ref[first + c:first + c + 1, :] for c in range(chunks)], axis=1)


def stats_kernel(cfg, ids_hbm, hid_hbm, cot_hbm, gam_hbm, bet_hbm, emb_hbm, w1_hbm, b1_hbm, w2_hbm,
                 e_ref, log_ref, y_out, lab_out, lse_out, dx_out, did_out, xh_out, part_out, w1_out, b1_out, w2_out,
                 ids_ref, hid_ref, cot_ref, gam_ref, bet_ref, w1_ref, b1_ref, w2_ref, ids_smem,
                 yt_ref, pack_src, pack_dst, dx_src, dx_dst, st_src, st_all, e32_ref, x_ref, part_src, part_all,
                 e_sem, in_sem, send_sem, pack_sem, dx_sem, st_sem, part_sem):
    stages, tps, toks, dim, vocab = cfg
    chunks = toks // LANES
    rank = lax.axis_index('tp')
    stage = lax.axis_index('pp')
    last = stages - 1
    helper = stages - 2
    full, tail = vocab // TILE - 1, vocab - (vocab // TILE - 1) * TILE
    e_copy = pltpu.make_async_copy(emb_hbm, e_ref, e_sem)
    pairs = ((hid_hbm, hid_ref), (ids_hbm, ids_ref), (gam_hbm, gam_ref), (bet_hbm, bet_ref), (cot_hbm, cot_ref), (ids_hbm, ids_smem), (w1_hbm, w1_ref), (b1_hbm, b1_ref), (w2_hbm, w2_ref))
    hid_ld, ids_ld, gam_ld, bet_ld, cot_ld, smem_ld, w1_ld, b1_ld, w2_ld = [pltpu.make_async_copy(a, b, in_sem.at[i]) for i, (a, b) in enumerate(pairs)]

    def fetch(*copies):
        for copy in copies:
            copy.start()

    def ready(*copies):
        for copy in copies:
            copy.wait()

    def remote(src, dst, ssem, rsem, to_stage, off=0):
        return pltpu.make_async_remote_copy(src, dst, ssem, rsem, device_id={'pp': to_stage, 'tp': lax.rem(rank + off, tps)}, device_id_type=MESH)

    def pack_copy(to_stage, idx, src=None):
        return remote(pack_src if src is None else src, pack_dst, send_sem.at[idx], pack_sem, to_stage)

    def dx_copy():
        return remote(dx_src, dx_dst, send_sem.at[0], dx_sem, last)

    def part_copy(off):
        return remote(part_src, part_all.at[rank], send_sem.at[off], part_sem.at[rank], 0, off)

    def greet():
        bar = pltpu.get_barrier_semaphore()
        for ds in range(stages):
            for off in range(tps):
                if ds or off:
                    pl.semaphore_signal(bar, inc=1, device_id={'pp': lax.rem(stage + ds, stages), 'tp': lax.rem(rank + off, tps)}, device_id_type=MESH)

    def met():
        pl.semaphore_wait(pltpu.get_barrier_semaphore(), stages * tps - 1)

    def normed(rows, gam, bet):
        hat, _ = ln_hat(rows)
        norm = (hat * gam + bet).astype(B)
        xh_out[...] = hat
        y_out[...] = norm
        yt_ref[...] = norm.astype(F).T.astype(B)

    def unpack():
        normed(pack_dst[0:toks, :], pack_dst[toks + chunks:toks + chunks + 1, :], pack_dst[toks + chunks + 1:toks + chunks + 2, :])
        lab_out[0:chunks, :] = pack_dst[toks:toks + chunks, :].astype(jnp.int32)

    def st_sends(which):
        slot = 2 * rank + which
        return [remote(st_src, st_all.at[slot], send_sem.at[2 + i], st_sem.at[slot], lax.rem(stage + ds, stages), off) for i, (ds, off) in enumerate((ds, off) for ds in range(stages) for off in range(tps) if ds or off)]

    def st_wait(slot):
        remote(st_src, st_all.at[slot], send_sem.at[0], st_sem.at[slot], last).wait_recv()

    def finish_stats():
        tops = [st_all[r, 0:chunks, :] for r in range(2 * tps)]
        sums = [st_all[r, chunks:2 * chunks, :] for r in range(2 * tps)]
        top = functools.reduce(jnp.maximum, tops)
        tot = functools.reduce(jnp.add, [s * jnp.exp(t - top) for s, t in zip(sums, tops)])
        lse_out[0:chunks, :] = top + jnp.log(tot)

    def logit_tile(row, size):
        logits = mm(e_ref[pl.ds(row, size), :], yt_ref[...])
        log_ref[pl.ds(row, size), :] = logits
        return logits

    def fill_logits(first, end):
        def step(i, carry):
            logit_tile(pl.multiple_of(i * TILE, TILE), TILE)
            return carry
        lax.fori_loop(first, end, step, 0, unroll=min(8, end - first))

    def logits_to(row, top, size=TILE):
        return jnp.maximum(top, jnp.max(logit_tile(row, size).reshape(size // 8, 8, toks), axis=0))

    def add_exp(row, top_old, top, tot, size=TILE):
        ex = jnp.exp(log_ref[pl.ds(row, size), :].reshape(size // 8, 8, toks) - top[None])
        return tot * jnp.exp(top_old - top) + jnp.sum(ex, axis=0)

    def begin_stats(first):
        low = jnp.full((8, toks), -jnp.inf, F)
        top = logits_to(first * TILE, low)
        return top, top, jnp.zeros((8, toks), F)

    def run_stats(first, end, carry):
        def step(i, carry):
            old, top, tot = carry
            row = pl.multiple_of(i * TILE, TILE)
            new = logits_to(row + TILE, top)
            return top, new, add_exp(row, old, top, tot)
        return lax.fori_loop(first, end, step, carry, unroll=min(8, end - first))

    def share_stats(top, tot, which):
        high = jnp.max(top, axis=0, keepdims=True)
        tot = jnp.sum(tot * jnp.exp(top - high), axis=0, keepdims=True)
        for c in range(chunks):
            st_src[c:c + 1, :] = high[:, c * LANES:(c + 1) * LANES]
            st_src[chunks + c:chunks + c + 1, :] = tot[:, c * LANES:(c + 1) * LANES]
        st_all[2 * rank + which] = st_src[...]
        sends = st_sends(which)
        for send in sends:
            send.start()
        return sends

    def mlp():
        ready(hid_ld, cot_ld, gam_ld, bet_ld, w1_ld, b1_ld, w2_ld)
        hat, _ = ln_hat(hid_ref[...].astype(F))
        norm = (hat * gam_ref[...] + bet_ref[...]).astype(B)
        pre = mm(norm, w1_ref[...]) + b1_ref[...]
        cube = 0.7978845608028654 * (pre + 0.044715 * (pre * pre * pre))
        th = jnp.tanh(cube)
        act = pre * (0.5 * (1.0 + th))
        slope = 0.5 * (1.0 + th) + pre * (0.5 * (1.0 - th * th)) * (0.7978845608028654 * (1.0 + 3 * 0.044715 * pre * pre))
        w2_out[...] = lax.dot_general(act.astype(B), cot_ref[...], TN, preferred_element_type=F)
        d_act = lax.dot_general(cot_ref[...], w2_ref[...], NT, preferred_element_type=F)
        d_pre = d_act * slope
        d_b = d_pre.astype(B)
        w1_out[...] = lax.dot_general(norm, d_b, TN, preferred_element_type=F)
        b1_out[...] = jnp.sum(d_pre, axis=0, keepdims=True)
        d_h = lax.dot_general(d_b, w1_ref[...], NT, preferred_element_type=F)
        part_out[0:1, :] = jnp.sum(d_h * hat, axis=0, keepdims=True)
        part_out[1:2, :] = jnp.sum(d_h, axis=0, keepdims=True)
        part_out[2:8, :] = jnp.zeros((6, LANES), F)

    @pl.when(stage == last)
    def _():
        fetch(hid_ld, ids_ld, gam_ld, bet_ld, e_copy)
        greet()
        ready(hid_ld, ids_ld, gam_ld, bet_ld)
        rows = hid_ref[...].astype(F)
        pack_src[0:toks, :] = rows
        pack_src[toks:toks + chunks, :] = ids_ref[...].astype(F)
        pack_src[toks + chunks:toks + chunks + 1, :] = gam_ref[...]
        pack_src[toks + chunks + 1:toks + chunks + 2, :] = bet_ref[...]
        normed(rows, gam_ref[...], bet_ref[...])
        lab_out[0:chunks, :] = ids_ref[...]
        e_copy.wait()
        carry = run_stats(0, EARLY, begin_stats(0))
        met()
        pack_copy(helper, 1).start()
        pack_copy(0, 0).start()
        old, top, tot = run_stats(EARLY, SPLIT_STATS - 1, carry)
        tot = add_exp((SPLIT_STATS - 1) * TILE, old, top, tot)
        sends = share_stats(top, tot, 0)
        fill_logits(SPLIT_STATS, full)
        logit_tile(full * TILE, tail)
        dx_copy().wait_recv()
        dx_out[...] = dx_dst[0:toks, :].astype(B)
        did_out[0:chunks, :] = dx_dst[toks:toks + chunks, :].astype(jnp.int32)
        st_wait(2 * rank + 1)
        for off in range(1, tps):
            st_wait(2 * lax.rem(rank + off, tps))
            st_wait(2 * lax.rem(rank + off, tps) + 1)
        finish_stats()
        pack_copy(helper, 1).wait_send()
        pack_copy(0, 0).wait_send()
        for send in sends:
            send.wait_send()

    @pl.when(stage == helper)
    def _():
        fetch(hid_ld, cot_ld, gam_ld, bet_ld, w1_ld, b1_ld, w2_ld, e_copy)
        greet()
        mlp()
        met()
        e_copy.wait()
        pack_copy(helper, 1).wait_recv()
        unpack()
        old, top, tot = run_stats(SPLIT_STATS, full - 1, begin_stats(SPLIT_STATS))
        new = logits_to(full * TILE, top, tail)
        tot = add_exp((full - 1) * TILE, old, top, tot)
        tot = add_exp(full * TILE, top, new, tot, tail)
        sends = share_stats(new, tot, 1)
        fill_logits(SPLIT_DY, SPLIT_STATS)
        st_wait(2 * rank)
        for off in range(1, tps):
            st_wait(2 * lax.rem(rank + off, tps))
            st_wait(2 * lax.rem(rank + off, tps) + 1)
        finish_stats()
        for send in sends:
            send.wait_send()

    @pl.when(stage == 0)
    def _():
        fetch(cot_ld, ids_ld, gam_ld, smem_ld, e_copy)
        greet()
        ready(cot_ld, ids_ld, gam_ld, smem_ld)
        e_copy.wait()

        def widen(i, carry):
            row = pl.multiple_of(i * TILE, TILE)
            e32_ref[pl.ds(row, TILE), :] = e_ref[pl.ds(row, TILE), :].astype(F)
            return carry

        lax.fori_loop(0, full, widen, 0, unroll=4)
        e32_ref[full * TILE:vocab, :] = e_ref[full * TILE:vocab, :].astype(F)
        base = rank * vocab
        for c in range(chunks):
            def pick(i, carry):
                row = jnp.clip(ids_smem[c, i] - base, 0, vocab - 1)
                x_ref[pl.ds(c * LANES + i, 1), :] = e32_ref[pl.ds(row, 1), :]
                return carry
            lax.fori_loop(0, LANES, pick, 0, unroll=16)
        local = lanes_row(ids_ref, 0, chunks) - base
        inside = jnp.where((local >= 0) & (local < vocab), 1.0, 0.0)
        mask = jnp.broadcast_to(inside, (LANES, toks)).T
        hat, inv = ln_hat(x_ref[...])
        cot = cot_ref[...].astype(F)
        scaled = cot * gam_ref[...]
        grad = inv * (scaled - jnp.mean(scaled, axis=-1, keepdims=True) - hat * jnp.mean(scaled * hat, axis=-1, keepdims=True))
        grad = jnp.where(mask > 0.5, grad, 0.0).astype(B)
        dx_out[...] = grad
        did_out[0:chunks, :] = ids_ref[...]
        dx_src[0:toks, :] = grad.astype(F)
        dx_src[toks:toks + chunks, :] = ids_ref[...].astype(F)
        part_src[0:1, :] = jnp.sum(jnp.where(mask > 0.5, cot * hat, 0.0), axis=0, keepdims=True)
        part_src[1:2, :] = jnp.sum(jnp.where(mask > 0.5, cot, 0.0), axis=0, keepdims=True)
        part_src[2:8, :] = jnp.zeros((6, LANES), F)
        part_all[rank] = part_src[...]
        met()
        dx_copy().start()
        for off in range(1, tps):
            part_copy(off).start()
        pack_copy(0, 0).wait_recv()
        pack_copy(1, 2 + tps, pack_dst).start()
        unpack()
        fill_logits(0, full)
        logit_tile(full * TILE, tail)
        for off in range(1, tps):
            src = lax.rem(rank + off, tps)
            remote(part_src, part_all.at[src], send_sem.at[0], part_sem.at[src], 0).wait_recv()
        part_out[...] = functools.reduce(jnp.add, [part_all[r] for r in range(tps)])
        for slot in range(2 * tps):
            st_wait(slot)
        finish_stats()
        dx_copy().wait_send()
        pack_copy(1, 2 + tps, pack_dst).wait_send()
        for off in range(1, tps):
            part_copy(off).wait_send()

    @pl.when((stage != 0) & (stage != helper) & (stage != last))
    def _():
        fetch(hid_ld, cot_ld, gam_ld, bet_ld, w1_ld, b1_ld, w2_ld, e_copy)
        greet()
        mlp()
        met()
        e_copy.wait()
        pack_copy(0, 0).wait_recv()
        unpack()
        fill_logits(0, SPLIT_DY)
        for slot in range(2 * tps):
            st_wait(slot)
        finish_stats()


def grad_kernel(cfg, e_ref, log_ref, y_ref, lab_ref, lse_ref, dx_ref, did_ref, xh_ref, pin_ref, w1_in, b1_in, w2_in,
                emb_out, w1_out, b1_out, w2_out, part_out, out_ref, dyt_ref, o_sem):
    stages, tps, toks, dim, vocab = cfg
    chunks = toks // LANES
    rank = lax.axis_index('tp')
    stage = lax.axis_index('pp')
    last = stages - 1
    helper = stages - 2
    base = rank * vocab
    full, tail = vocab // TILE - 1, vocab - (vocab // TILE - 1) * TILE
    group = 16
    groups = full // group
    size16 = group * TILE

    @pl.when((stage == 0) | (stage == last))
    def _():
        w1_out[...] = jnp.zeros(w1_out.shape, F)
        b1_out[...] = jnp.zeros(b1_out.shape, F)
        w2_out[...] = jnp.zeros(w2_out.shape, F)
        part_out[...] = pin_ref[...]
        lse = lanes_row(lse_ref, 0, chunks)
        lab = (lanes_row(lab_ref, 0, chunks) - base)
        did = (lanes_row(did_ref, 0, chunks) - base)
        lab = jnp.where((lab >= 0) & (lab < vocab), lab, -1).astype(jnp.int16)
        did = jnp.where((did >= 0) & (did < vocab), did, -1).astype(jnp.int16)

        def out_copy(c):
            size = tail if c == groups else size16
            return pltpu.make_async_copy(out_ref.at[pl.ds(c * size16, size)], emb_out.at[pl.ds(c * size16, size)], o_sem.at[c])

        def work(row, size):
            p = jnp.exp2((log_ref[pl.ds(row, size), :] - lse) * LOG2E)
            rows = (lax.broadcasted_iota(jnp.int32, (size, LANES), 0) + row).astype(jnp.int16)
            one, zero = jnp.ones((size, LANES), B), jnp.zeros((size, LANES), B)
            g, h = [], []
            for c in range(chunks):
                cols = slice(c * LANES, (c + 1) * LANES)
                pc = p[:, cols]
                g.append(jnp.where(rows == lab[:, cols], (pc - 1.0).astype(B), pc.astype(B)))
                h.append(jnp.where(rows == did[:, cols], one, zero))
            out_ref[pl.ds(row, size), :] = mm(jnp.concatenate(g, axis=1), y_ref[...]) + mm(jnp.concatenate(h, axis=1), dx_ref[...])

        for c in range(groups):
            def step(i, carry):
                work(pl.multiple_of(c * size16 + i * TILE, TILE), TILE)
                return carry
            lax.fori_loop(0, group, step, 0, unroll=16)
            out_copy(c).start()
        work(full * TILE, tail)
        out_copy(groups).start()
        for c in range(groups + 1):
            out_copy(c).wait()

    @pl.when((stage != 0) & (stage != last))
    def _():
        out_ref[0:size16, :] = jnp.zeros((size16, dim), F)

        def zero_copy(c):
            n = tail if c == groups else size16
            return pltpu.make_async_copy(out_ref.at[pl.ds(0, n)], emb_out.at[pl.ds(c * size16, n)], o_sem.at[c])

        for c in range(groups + 1):
            zero_copy(c).start()
        w1_out[...] = w1_in[...]
        b1_out[...] = b1_in[...]
        w2_out[...] = w2_in[...]
        part_out[...] = pin_ref[...]
        lse = lanes_row(lse_ref, 0, chunks)
        lab = lanes_row(lab_ref, 0, chunks) - base
        dyt_ref[...] = jnp.zeros((dim, toks), F)

        def work(row, size, loss):
            x = log_ref[pl.ds(row, size), :] - lse
            p = jnp.exp2(x * LOG2E)
            rows = lax.broadcasted_iota(jnp.int32, (size, LANES), 0) + row
            g, picked = [], []
            for c in range(chunks):
                cols = slice(c * LANES, (c + 1) * LANES)
                hit = rows == lab[:, cols]
                pc = p[:, cols]
                g.append(jnp.where(hit, pc - 1.0, pc).astype(B))
                picked.append(jnp.sum(jnp.where(hit, x[:, cols], 0.0).reshape(size // 8, 8, LANES), axis=0))
            dyt_ref[...] += lax.dot_general(e_ref[pl.ds(row, size), :], jnp.concatenate(g, axis=1), TN, preferred_element_type=F)
            return loss + functools.reduce(jnp.add, picked)

        def sweep(first, end, loss):
            def step(i, loss):
                return work(pl.multiple_of(i * TILE, TILE), TILE, loss)
            return lax.fori_loop(first, end, step, loss, unroll=min(8, end - first))

        def finish(loss):
            dy = dyt_ref[...].T
            part_out[2:3, :] = jnp.sum(dy * xh_ref[...], axis=0, keepdims=True)
            part_out[3:4, :] = jnp.sum(dy, axis=0, keepdims=True)
            part_out[4:5, :] = jnp.sum(loss, axis=0, keepdims=True)

        @pl.when(stage == helper)
        def _():
            loss = sweep(SPLIT_DY, full, jnp.zeros((8, LANES), F))
            finish(work(full * TILE, tail, loss))

        @pl.when(stage != helper)
        def _():
            finish(sweep(0, SPLIT_DY, jnp.zeros((8, LANES), F)))

        for c in range(groups + 1):
            zero_copy(c).wait()


def sum_kernel(cfg, part_ref, sum_out, got, send_sem, recv_sem):
    stages, tps, toks, dim, vocab = cfg
    rank = lax.axis_index('tp')
    stage = lax.axis_index('pp')
    last = stages - 1
    helper = stages - 2
    mids = helper
    bar = pltpu.get_barrier_semaphore()

    def copy_to(to_stage, off, idx):
        slot = (stage - 1) * tps + rank
        return pltpu.make_async_remote_copy(part_ref, got.at[slot], send_sem.at[idx], recv_sem.at[slot], device_id={'pp': to_stage, 'tp': lax.rem(rank + off, tps)}, device_id_type=MESH)

    def arrived(slot):
        return pltpu.make_async_remote_copy(part_ref, got.at[slot], send_sem.at[0], recv_sem.at[slot], device_id={'tp': rank}, device_id_type=MESH)

    def total(at):
        return functools.reduce(jnp.add, [got[at * tps + r] for r in range(tps)])

    @pl.when((stage != 0) & (stage != last))
    def _():
        for to_stage in range(1, 1 + mids):
            for off in range(tps):
                @pl.when((stage != to_stage) | (off != 0))
                def _():
                    pl.semaphore_signal(bar, inc=1, device_id={'pp': to_stage, 'tp': lax.rem(rank + off, tps)}, device_id_type=MESH)
        pl.semaphore_wait(bar, mids * tps - 1)

        @pl.when(stage == helper)
        def _():
            sends = [copy_to(helper, off, off) for off in range(1, tps)]
            for send in sends:
                send.start()
            got[(helper - 1) * tps + rank] = part_ref[...]
            for at in range(helper - 1):
                for r in range(tps):
                    arrived(at * tps + r).wait_recv()
            for off in range(1, tps):
                arrived((helper - 1) * tps + lax.rem(rank + off, tps)).wait_recv()
            own = total(helper - 1)
            rest = functools.reduce(jnp.add, [total(at) for at in range(helper)])
            sum_out[...] = jnp.concatenate([own[0:2, :], rest[2:8, :]], axis=0)
            for send in sends:
                send.wait_send()

        @pl.when(stage != helper)
        def _():
            sends = [copy_to(helper, off, tps + off) for off in range(tps)] + [copy_to(stage, off, off) for off in range(1, tps)]
            for send in sends:
                send.start()
            mine = (stage - 1) * tps
            got[mine + rank] = part_ref[...]
            for off in range(1, tps):
                arrived(mine + lax.rem(rank + off, tps)).wait_recv()
            sum_out[...] = functools.reduce(jnp.add, [got[mine + r] for r in range(tps)])
            for send in sends:
                send.wait_send()

    @pl.when((stage == 0) | (stage == last))
    def _():
        sum_out[...] = part_ref[...]


def hand_kernel(cfg, sum_ref, gam_out, bet_out, loss_out, got, send_sem, recv_sem):
    stages, tps, toks, dim, vocab = cfg
    stage = lax.axis_index('pp')
    last = stages - 1
    helper = stages - 2
    bar = pltpu.get_barrier_semaphore()

    def hand_over():
        return pltpu.make_async_remote_copy(sum_ref, got, send_sem, recv_sem, device_id={'pp': last}, device_id_type=MESH)

    @pl.when(stage == helper)
    def _():
        pl.semaphore_signal(bar, inc=1, device_id={'pp': last}, device_id_type=MESH)
        pl.semaphore_wait(bar, 1)
        hand_over().start()
        hand_over().wait_send()

    @pl.when(stage != last)
    def _():
        gam_out[...] = sum_ref[0:1, :]
        bet_out[...] = sum_ref[1:2, :]
        loss_out[...] = jnp.zeros((1, 1), F)

    @pl.when(stage == last)
    def _():
        pl.semaphore_signal(bar, inc=1, device_id={'pp': helper}, device_id_type=MESH)
        pl.semaphore_wait(bar, 1)
        hand_over().wait_recv()
        gam_out[...] = got[2:3, :]
        bet_out[...] = got[3:4, :]
        loss_out[...] = jnp.sum(got[4:5, :], axis=1, keepdims=True) * (-1.0 / toks)


def solution(mesh):
    stages, tps = mesh.shape['pp'], mesh.shape['tp']
    lead = ('dp', 'pp')
    hbm = pl.BlockSpec(memory_space=pltpu.HBM)
    vmem = pl.BlockSpec(memory_space=pltpu.VMEM)
    S = jax.ShapeDtypeStruct
    V = pltpu.VMEM
    DMA = pltpu.SemaphoreType.DMA
    I = jnp.int32

    def stay(*arrays):
        return [pltpu.with_memory_space_constraint(a, pltpu.HBM) for a in arrays]

    def body(tok_ids, hid_in, cot_in, ln_gamma, ln_beta, emb_table, w_in, b_in, w_out):
        dim = hid_in.shape[-1]
        hid = hid_in.reshape(-1, dim)
        cot = cot_in.reshape(-1, dim)
        toks = hid.shape[0]
        chunks = toks // LANES
        ids = tok_ids.reshape(chunks, LANES)
        table = emb_table[0]
        vocab = table.shape[0]
        ff = w_in.shape[2]
        cfg = (stages, tps, toks, dim, vocab)
        rows = toks + 2 * chunks
        vec = S((8, LANES), F)
        weights = (S((dim, ff), F), S((1, ff), F), S((ff, dim), F))
        mids = pl.pallas_call(
            functools.partial(stats_kernel, cfg), name='stats',
            out_shape=(S((vocab, dim), B), S((vocab, toks), F), S((toks, dim), B), S((8, LANES), I), vec, S((toks, dim), B), S((8, LANES), I), S((toks, dim), F), vec) + weights,
            in_specs=[hbm] * 9, out_specs=[vmem] * 12,
            scratch_shapes=[
                V((chunks, LANES), I), V((toks, dim), B), V((toks, dim), B), V((1, dim), F), V((1, dim), F), V((dim, ff), B), V((1, ff), F), V((ff, dim), B), pltpu.SMEM((chunks, LANES), I),
                V((dim, toks), B), V((rows, dim), F), V((rows, dim), F), V((rows, dim), F), V((rows, dim), F),
                V((8, LANES), F), V((2 * tps, 8, LANES), F), V((vocab, dim), F), V((toks, dim), F), V((8, LANES), F), V((tps, 8, LANES), F),
                DMA, DMA((9,)), DMA((2 + stages * tps,)), DMA, DMA, DMA((2 * tps,)), DMA((tps,))],
            compiler_params=pltpu.CompilerParams(collective_id=0, has_side_effects=True, vmem_limit_bytes=GRANT),
        )(*stay(ids, hid, cot, ln_gamma, ln_beta, table, w_in[0], b_in, w_out[0]))
        groups = (vocab // TILE - 1) // 16 + 1
        emb_grad, w1g, b1g, w2g, part = pl.pallas_call(
            functools.partial(grad_kernel, cfg), name='grads',
            out_shape=(S((vocab, dim), F),) + weights + (vec,),
            in_specs=[vmem] * 12, out_specs=[hbm] + [vmem] * 4,
            scratch_shapes=[V((vocab, dim), F), V((dim, toks), F), DMA((groups,))],
            compiler_params=pltpu.CompilerParams(vmem_limit_bytes=GRANT),
        )(*mids)
        sums = pl.pallas_call(
            functools.partial(sum_kernel, cfg), name='sums', out_shape=vec, in_specs=[vmem], out_specs=vmem,
            scratch_shapes=[V(((stages - 2) * tps, 8, LANES), F), DMA((2 * tps,)), DMA(((stages - 2) * tps,))],
            compiler_params=pltpu.CompilerParams(collective_id=1, has_side_effects=True, vmem_limit_bytes=4 << 20),
        )(part)
        gam, bet, loss = pl.pallas_call(
            functools.partial(hand_kernel, cfg), name='hand',
            out_shape=(S((1, dim), F), S((1, dim), F), S((1, 1), F)), in_specs=[vmem], out_specs=[vmem] * 3,
            scratch_shapes=[V((8, LANES), F), DMA, DMA],
            compiler_params=pltpu.CompilerParams(collective_id=2, has_side_effects=True, vmem_limit_bytes=4 << 20),
        )(sums)
        return emb_grad[None], loss.reshape(1), gam, bet, w1g[None], b1g, w2g[None]

    specs_in = (P(lead, None, None), P(lead, None, None, None), P(lead, None, None, None), P(lead, None), P(lead, None), P(lead, 'tp', None), P(lead, None, 'tp'), P(lead, 'tp'), P(lead, 'tp', None))
    specs_out = (P(lead, 'tp', None), P(lead), P(lead, None), P(lead, None), P(lead, None, 'tp'), P(lead, 'tp'), P(lead, 'tp', None))
    return jax.shard_map(body, mesh=mesh, in_specs=specs_in, out_specs=specs_out, check_vma=False)
```

```python
import functools

import jax
import jax.numpy as jnp
from jax import lax
from jax.experimental import pallas as pl
from jax.experimental.pallas import tpu as pltpu
from jax.sharding import PartitionSpec as P

F = jnp.float32
B = jnp.bfloat16
LN_EPS = 1e-5
LOG2E = 1.4426950408889634
LANES = 128
TILE = 256
SPLIT_STATS = 35
SPLIT_DY = 26
EARLY = 4
FIRST = 32
PARTS = 4
DY_LATE = 14
GRANT = 14 << 20
MESH = pl.DeviceIdType.MESH
NT = (((1,), (1,)), ((), ()))
TN = (((0,), (0,)), ((), ()))


def ln_hat(rows):
    centre = rows - jnp.mean(rows, axis=-1, keepdims=True)
    inv = lax.rsqrt(jnp.mean(centre * centre, axis=-1, keepdims=True) + LN_EPS)
    return centre * inv, inv


def tile_ids(row, size):
    return (lax.broadcasted_iota(jnp.int32, (size, LANES), 0) + row).astype(jnp.int16)


def local_ids(ref, chunks, base, vocab):
    ids = lanes_row(ref, 0, chunks) - base
    return jnp.where((ids >= 0) & (ids < vocab), ids, -1).astype(jnp.int16)


def steps(count):
    return max(d for d in range(1, 14) if count % d == 0)


def mm(a, b):
    return jnp.dot(a, b, preferred_element_type=F)


def lanes_row(ref, first, chunks):
    return jnp.concatenate([ref[first + c:first + c + 1, :] for c in range(chunks)], axis=1)


def stats_kernel(cfg, ids_hbm, hid_hbm, cot_hbm, gam_hbm, bet_hbm, emb_hbm, w1_hbm, b1_hbm, w2_hbm,
                 e_ref, log_ref, first_ref, y_out, lab_out, lse_out, dx_out, did_out, xh_out, part_out, w1_out, b1_out, w2_out,
                 ids_ref, hid_ref, cot_ref, gam_ref, bet_ref, w1_ref, b1_ref, w2_ref, ids_smem,
                 yt_ref, buf, pack_src, pack_dst, dx_src, dx_dst, st_src, st_all, e32_ref, x_ref, part_src, part_all,
                 e_sem, in_sem, send_sem, pack_sem, dx_sem, st_sem, part_sem):
    stages, tps, toks, dim, vocab = cfg
    chunks = toks // LANES
    rank = lax.axis_index('tp')
    stage = lax.axis_index('pp')
    last = stages - 1
    helper = stages - 2
    full, tail = vocab // TILE - 1, vocab - (vocab // TILE - 1) * TILE
    vecs = 2 * chunks
    half = toks // 2
    cuts = [i * (full // PARTS) for i in range(PARTS)] + [full]

    def e_part(i):
        start = cuts[i] * TILE
        size = (vocab if i == PARTS - 1 else cuts[i + 1] * TILE) - start
        return pltpu.make_async_copy(emb_hbm.at[pl.ds(start, size)], e_ref.at[pl.ds(start, size)], e_sem.at[i])

    e_parts = [e_part(i) for i in range(PARTS)]
    pairs = ((hid_hbm, hid_ref), (ids_hbm, ids_ref), (gam_hbm, gam_ref), (bet_hbm, bet_ref), (cot_hbm, cot_ref), (ids_hbm, ids_smem), (w1_hbm, w1_ref), (b1_hbm, b1_ref), (w2_hbm, w2_ref))
    hid_ld, ids_ld, gam_ld, bet_ld, cot_ld, smem_ld, w1_ld, b1_ld, w2_ld = [pltpu.make_async_copy(a, b, in_sem.at[i]) for i, (a, b) in enumerate(pairs)]

    def fetch(*copies):
        for copy in copies:
            copy.start()

    def ready(*copies):
        for copy in copies:
            copy.wait()

    def remote(src, dst, ssem, rsem, to_stage, off=0):
        return pltpu.make_async_remote_copy(src, dst, ssem, rsem, device_id={'pp': to_stage, 'tp': lax.rem(rank + off, tps)}, device_id_type=MESH)

    def pack_rows(which):
        return pl.ds(0, vecs + half) if which == 0 else pl.ds(vecs + half, half)

    def pack_copy(to_stage, which, idx, src):
        return remote(src.at[pack_rows(which)], pack_dst.at[pack_rows(which)], send_sem.at[idx], pack_sem.at[which], to_stage)

    def pack_sends():
        return [pack_copy(helper, 0, 0, pack_src), pack_copy(helper, 1, 1, pack_src), pack_copy(0, 0, 2, pack_src), pack_copy(0, 1, 3, pack_src)]

    def relays():
        return [pack_copy(1, w, 2 + tps + w, pack_dst) for w in range(2)]

    def dx_copy():
        return remote(dx_src, dx_dst, send_sem.at[0], dx_sem, last)

    def part_copy(off):
        return remote(part_src, part_all.at[rank], send_sem.at[off], part_sem.at[rank], 0, off)

    def greet():
        bar = pltpu.get_barrier_semaphore()
        for ds in range(stages):
            for off in range(tps):
                if ds or off:
                    pl.semaphore_signal(bar, inc=1, device_id={'pp': lax.rem(stage + ds, stages), 'tp': lax.rem(rank + off, tps)}, device_id_type=MESH)

    def met():
        pl.semaphore_wait(pltpu.get_barrier_semaphore(), stages * tps - 1)

    def normed(rows, gam, bet, start, size):
        hat, _ = ln_hat(rows)
        norm = (hat * gam + bet).astype(B)
        xh_out[start:start + size, :] = hat
        y_out[start:start + size, :] = norm
        yt_ref[:, start:start + size] = norm.astype(F).T.astype(B)

    def unpack(which):
        start = which * half
        normed(pack_dst[vecs + start:vecs + start + half, :], pack_dst[chunks:chunks + 1, :], pack_dst[chunks + 1:chunks + 2, :], start, half)
        if which == 0:
            lab_out[0:chunks, :] = pack_dst[0:chunks, :].astype(jnp.int32)

    def unpack_all():
        for w in range(2):
            pack_copy(helper, w, 0, pack_src).wait_recv()
            unpack(w)

    def st_sends(which):
        slot = 2 * rank + which
        return [remote(st_src, st_all.at[slot], send_sem.at[4 + i], st_sem.at[slot], lax.rem(stage + ds, stages), off) for i, (ds, off) in enumerate((ds, off) for ds in range(stages) for off in range(tps) if ds or off)]

    def st_wait(slot):
        remote(st_src, st_all.at[slot], send_sem.at[0], st_sem.at[slot], last).wait_recv()

    def finish_stats():
        tops = [st_all[r, 0:chunks, :] for r in range(2 * tps)]
        sums = [st_all[r, chunks:2 * chunks, :] for r in range(2 * tps)]
        top = functools.reduce(jnp.maximum, tops)
        tot = functools.reduce(jnp.add, [s * jnp.exp(t - top) for s, t in zip(sums, tops)])
        lse_out[0:chunks, :] = top + jnp.log(tot)

    def logit_tile(row, size):
        logits = mm(e_ref[pl.ds(row, size), :], yt_ref[...])
        log_ref[pl.ds(row, size), :] = logits
        return logits

    def fill_logits(first, end):
        def step(i, carry):
            logit_tile(pl.multiple_of(i * TILE, TILE), TILE)
            return carry
        lax.fori_loop(first, end, step, 0, unroll=steps(end - first))

    def first_tiles(first, end):
        did = local_ids(did_out, chunks, rank * vocab, vocab)

        def fill(row, size):
            rows = tile_ids(row, size)
            one, zero = jnp.ones((size, LANES), B), jnp.zeros((size, LANES), B)
            h = [jnp.where(rows == did[:, c * LANES:(c + 1) * LANES], one, zero) for c in range(chunks)]
            first_ref[pl.ds(row, size), :] = mm(jnp.concatenate(h, axis=1), dx_out[...])

        def step(i, carry):
            fill(pl.multiple_of(i * TILE, TILE), TILE)
            return carry
        lax.fori_loop(first, end, step, 0, unroll=steps(end - first))
        if end == full:
            fill(full * TILE, tail)

    def logits_to(row, slot, top, size=TILE):
        logits = logit_tile(row, size)
        buf[slot, 0:size] = logits
        return jnp.maximum(top, jnp.max(logits.reshape(size // 8, 8, toks), axis=0))

    def add_exp(slot, top_old, top, tot, size=TILE):
        ex = jnp.exp(buf[slot, 0:size].reshape(size // 8, 8, toks) - top[None])
        return tot * jnp.exp(top_old - top) + jnp.sum(ex, axis=0)

    def begin_stats(first):
        low = jnp.full((8, toks), -jnp.inf, F)
        top = logits_to(first * TILE, 0, low)
        return top, top, jnp.zeros((8, toks), F)

    def run_stats(first, pairs, carry):
        def step(i, carry):
            old, top, tot = carry
            row = pl.multiple_of(first * TILE + i * 2 * TILE, TILE)
            mid = logits_to(row + TILE, 1, top)
            tot = add_exp(0, old, top, tot)
            new = logits_to(row + 2 * TILE, 0, mid)
            tot = add_exp(1, top, mid, tot)
            return mid, new, tot
        return lax.fori_loop(0, pairs, step, carry, unroll=min(steps(pairs), 6))

    def share_stats(top, tot, which):
        high = jnp.max(top, axis=0, keepdims=True)
        tot = jnp.sum(tot * jnp.exp(top - high), axis=0, keepdims=True)
        for c in range(chunks):
            st_src[c:c + 1, :] = high[:, c * LANES:(c + 1) * LANES]
            st_src[chunks + c:chunks + c + 1, :] = tot[:, c * LANES:(c + 1) * LANES]
        st_all[2 * rank + which] = st_src[...]
        sends = st_sends(which)
        for send in sends:
            send.start()
        return sends

    def mlp():
        ready(hid_ld, cot_ld, gam_ld, bet_ld, w1_ld, b1_ld, w2_ld)
        hat, _ = ln_hat(hid_ref[...].astype(F))
        norm = (hat * gam_ref[...] + bet_ref[...]).astype(B)
        pre = mm(norm, w1_ref[...]) + b1_ref[...]
        cube = 0.7978845608028654 * (pre + 0.044715 * (pre * pre * pre))
        th = jnp.tanh(cube)
        act = pre * (0.5 * (1.0 + th))
        slope = 0.5 * (1.0 + th) + pre * (0.5 * (1.0 - th * th)) * (0.7978845608028654 * (1.0 + 3 * 0.044715 * pre * pre))
        w2_out[...] = lax.dot_general(act.astype(B), cot_ref[...], TN, preferred_element_type=F)
        d_act = lax.dot_general(cot_ref[...], w2_ref[...], NT, preferred_element_type=F)
        d_pre = d_act * slope
        d_b = d_pre.astype(B)
        w1_out[...] = lax.dot_general(norm, d_b, TN, preferred_element_type=F)
        b1_out[...] = jnp.sum(d_pre, axis=0, keepdims=True)
        d_h = lax.dot_general(d_b, w1_ref[...], NT, preferred_element_type=F)
        part_out[0:1, :] = jnp.sum(d_h * hat, axis=0, keepdims=True)
        part_out[1:2, :] = jnp.sum(d_h, axis=0, keepdims=True)
        part_out[2:8, :] = jnp.zeros((6, LANES), F)

    @pl.when(stage == last)
    def _():
        fetch(hid_ld, ids_ld, gam_ld, bet_ld, *e_parts)
        greet()
        ready(hid_ld, ids_ld, gam_ld, bet_ld)
        rows = hid_ref[...].astype(F)
        pack_src[vecs:vecs + toks, :] = rows
        pack_src[0:chunks, :] = ids_ref[...].astype(F)
        pack_src[chunks:chunks + 1, :] = gam_ref[...]
        pack_src[chunks + 1:chunks + 2, :] = bet_ref[...]
        pack_src[chunks + 2:vecs, :] = jnp.zeros((vecs - chunks - 2, dim), F)
        normed(rows, gam_ref[...], bet_ref[...], 0, toks)
        lab_out[0:chunks, :] = ids_ref[...]
        e_parts[0].wait()
        carry = run_stats(0, EARLY // 2, begin_stats(0))
        met()
        packs = pack_sends()
        for send in packs:
            send.start()
        ready(*e_parts[1:])
        old, top, tot = run_stats(EARLY, (SPLIT_STATS - 1 - EARLY) // 2, carry)
        tot = add_exp(0, old, top, tot)
        sends = share_stats(top, tot, 0)
        fill_logits(SPLIT_STATS, full)
        logit_tile(full * TILE, tail)
        dx_copy().wait_recv()
        dx_out[...] = dx_dst[0:toks, :].astype(B)
        did_out[0:chunks, :] = dx_dst[toks:toks + chunks, :].astype(jnp.int32)
        first_tiles(0, FIRST)
        st_wait(2 * rank + 1)
        for off in range(1, tps):
            st_wait(2 * lax.rem(rank + off, tps))
            st_wait(2 * lax.rem(rank + off, tps) + 1)
        finish_stats()
        for send in packs:
            send.wait_send()
        for send in sends:
            send.wait_send()

    @pl.when(stage == helper)
    def _():
        fetch(hid_ld, cot_ld, gam_ld, bet_ld, w1_ld, b1_ld, w2_ld, *e_parts)
        greet()
        mlp()
        met()
        ready(*e_parts)
        unpack_all()
        old, top, tot = run_stats(SPLIT_STATS, (full - 1 - SPLIT_STATS) // 2, begin_stats(SPLIT_STATS))
        new = logits_to(full * TILE, 1, top, tail)
        tot = add_exp(0, old, top, tot)
        tot = add_exp(1, top, new, tot, tail)
        sends = share_stats(new, tot, 1)
        fill_logits(SPLIT_DY, SPLIT_STATS)
        st_wait(2 * rank)
        for off in range(1, tps):
            st_wait(2 * lax.rem(rank + off, tps))
            st_wait(2 * lax.rem(rank + off, tps) + 1)
        finish_stats()
        for send in sends:
            send.wait_send()

    @pl.when(stage == 0)
    def _():
        fetch(cot_ld, ids_ld, gam_ld, smem_ld, *e_parts)
        greet()
        ready(cot_ld, ids_ld, gam_ld, smem_ld)

        def widen(i, carry):
            row = pl.multiple_of(i * TILE, TILE)
            e32_ref[pl.ds(row, TILE), :] = e_ref[pl.ds(row, TILE), :].astype(F)
            return carry

        for i in range(PARTS):
            e_parts[i].wait()
            lax.fori_loop(cuts[i], cuts[i + 1], widen, 0, unroll=4)
        e32_ref[full * TILE:vocab, :] = e_ref[full * TILE:vocab, :].astype(F)
        base = rank * vocab
        for c in range(chunks):
            def pick(i, carry):
                row = jnp.clip(ids_smem[c, i] - base, 0, vocab - 1)
                x_ref[pl.ds(c * LANES + i, 1), :] = e32_ref[pl.ds(row, 1), :]
                return carry
            lax.fori_loop(0, LANES, pick, 0, unroll=16)
        local = lanes_row(ids_ref, 0, chunks) - base
        inside = jnp.where((local >= 0) & (local < vocab), 1.0, 0.0)
        mask = jnp.broadcast_to(inside, (LANES, toks)).T
        hat, inv = ln_hat(x_ref[...])
        cot = cot_ref[...].astype(F)
        scaled = cot * gam_ref[...]
        grad = inv * (scaled - jnp.mean(scaled, axis=-1, keepdims=True) - hat * jnp.mean(scaled * hat, axis=-1, keepdims=True))
        grad = jnp.where(mask > 0.5, grad, 0.0).astype(B)
        dx_out[...] = grad
        did_out[0:chunks, :] = ids_ref[...]
        dx_src[0:toks, :] = grad.astype(F)
        dx_src[toks:toks + chunks, :] = ids_ref[...].astype(F)
        part_src[0:1, :] = jnp.sum(jnp.where(mask > 0.5, cot * hat, 0.0), axis=0, keepdims=True)
        part_src[1:2, :] = jnp.sum(jnp.where(mask > 0.5, cot, 0.0), axis=0, keepdims=True)
        part_src[2:8, :] = jnp.zeros((6, LANES), F)
        part_all[rank] = part_src[...]
        first_tiles(0, FIRST // 2)
        met()
        dx_copy().start()
        for off in range(1, tps):
            part_copy(off).start()
        first_tiles(FIRST // 2, full)
        sends = relays()
        for w in range(2):
            pack_copy(0, w, 0, pack_src).wait_recv()
            sends[w].start()
            unpack(w)
        fill_logits(0, full)
        logit_tile(full * TILE, tail)
        for off in range(1, tps):
            src = lax.rem(rank + off, tps)
            remote(part_src, part_all.at[src], send_sem.at[0], part_sem.at[src], 0).wait_recv()
        part_out[...] = functools.reduce(jnp.add, [part_all[r] for r in range(tps)])
        for slot in range(2 * tps):
            st_wait(slot)
        finish_stats()
        dx_copy().wait_send()
        for send in sends:
            send.wait_send()
        for off in range(1, tps):
            part_copy(off).wait_send()

    @pl.when((stage != 0) & (stage != helper) & (stage != last))
    def _():
        fetch(hid_ld, cot_ld, gam_ld, bet_ld, w1_ld, b1_ld, w2_ld, *e_parts)
        greet()
        mlp()
        met()
        ready(*e_parts)
        unpack_all()
        fill_logits(0, SPLIT_DY)
        for slot in range(2 * tps):
            st_wait(slot)
        finish_stats()


def dy_piece(cfg, e_ref, log_ref, lab_ref, lse_ref, xh_ref, dyt_ref, part_ref, first, end, with_tail):
    stages, tps, toks, dim, vocab = cfg
    chunks = toks // LANES
    full, tail = vocab // TILE - 1, vocab - (vocab // TILE - 1) * TILE
    lse = lanes_row(lse_ref, 0, chunks)
    lab = lanes_row(lab_ref, 0, chunks) - lax.axis_index('tp') * vocab
    dyt_ref[...] = jnp.zeros((dim, toks), F)

    def work(row, size, seen):
        x = log_ref[pl.ds(row, size), :] - lse
        p = jnp.exp2(x * LOG2E)
        rows = lax.broadcasted_iota(jnp.int32, (size, LANES), 0) + row
        g, found = [], []
        for c in range(chunks):
            cols = slice(c * LANES, (c + 1) * LANES)
            hit = rows == lab[:, cols]
            pc, xc, at = p[:, cols], x[:, cols], seen[c]
            g.append(jnp.where(hit, pc - 1.0, pc).astype(B))
            for k in range(0, size, 8):
                at = jnp.where(hit[k:k + 8, :], xc[k:k + 8, :], at)
            found.append(at)
        dyt_ref[...] += lax.dot_general(e_ref[pl.ds(row, size), :], jnp.concatenate(g, axis=1), TN, preferred_element_type=F)
        return tuple(found)

    def step(i, seen):
        return work(pl.multiple_of(i * TILE, TILE), TILE, seen)

    seen = lax.fori_loop(first, end, step, tuple(jnp.zeros((8, LANES), F) for _ in range(chunks)), unroll=steps(end - first))
    if with_tail:
        seen = work(full * TILE, tail, seen)
    loss = functools.reduce(jnp.add, seen)
    dy = dyt_ref[...].T
    part_ref[2:3, :] += jnp.sum(dy * xh_ref[...], axis=0, keepdims=True)
    part_ref[3:4, :] += jnp.sum(dy, axis=0, keepdims=True)
    part_ref[4:5, :] += jnp.sum(loss, axis=0, keepdims=True)


def grad_kernel(cfg, e_ref, log_ref, first_ref, y_ref, lab_ref, lse_ref, dx_ref, did_ref, xh_ref, pin_ref, w1_in, b1_in, w2_in,
                emb_out, w1_out, b1_out, w2_out, part_out, out_ref, dyt_ref, o_sem):
    stages, tps, toks, dim, vocab = cfg
    chunks = toks // LANES
    rank = lax.axis_index('tp')
    stage = lax.axis_index('pp')
    last = stages - 1
    helper = stages - 2
    base = rank * vocab
    full, tail = vocab // TILE - 1, vocab - (vocab // TILE - 1) * TILE
    group = 16
    groups = full // group
    size16 = group * TILE

    @pl.when((stage == 0) | (stage == last))
    def _():
        w1_out[...] = jnp.zeros(w1_out.shape, F)
        b1_out[...] = jnp.zeros(b1_out.shape, F)
        w2_out[...] = jnp.zeros(w2_out.shape, F)
        part_out[...] = pin_ref[...]
        lse = lanes_row(lse_ref, 0, chunks)
        lab = local_ids(lab_ref, chunks, base, vocab)
        did = local_ids(did_ref, chunks, base, vocab)

        def out_copy(c):
            size = tail if c == groups else size16
            return pltpu.make_async_copy(out_ref.at[pl.ds(c * size16, size)], emb_out.at[pl.ds(c * size16, size)], o_sem.at[c])

        def work(row, size, pick):
            p = jnp.exp2((log_ref[pl.ds(row, size), :] - lse) * LOG2E)
            rows = tile_ids(row, size)
            one, zero = jnp.ones((size, LANES), B), jnp.zeros((size, LANES), B)
            g, h = [], []
            for c in range(chunks):
                cols = slice(c * LANES, (c + 1) * LANES)
                pc = p[:, cols]
                g.append(jnp.where(rows == lab[:, cols], (pc - 1.0).astype(B), pc.astype(B)))
                if pick:
                    h.append(jnp.where(rows == did[:, cols], one, zero))
            first = mm(jnp.concatenate(h, axis=1), dx_ref[...]) if pick else first_ref[pl.ds(row, size), :]
            out_ref[pl.ds(row, size), :] = first + mm(jnp.concatenate(g, axis=1), y_ref[...])

        def sweep(first, end, pick):
            def step(i, carry):
                work(pl.multiple_of(i * TILE, TILE), TILE, pick)
                return carry
            lax.fori_loop(first, end, step, 0, unroll=steps(end - first) if pick else 16)

        for c in range(groups):
            if (c + 1) * group <= FIRST:
                sweep(c * group, (c + 1) * group, False)
            else:
                @pl.when(stage == 0)
                def _():
                    sweep(c * group, (c + 1) * group, False)
                    if c == groups - 1:
                        work(full * TILE, tail, False)

                @pl.when(stage != 0)
                def _():
                    sweep(c * group, (c + 1) * group, True)
                    if c == groups - 1:
                        work(full * TILE, tail, True)
            out_copy(c).start()
        out_copy(groups).start()
        for c in range(groups + 1):
            out_copy(c).wait()

    @pl.when((stage != 0) & (stage != last))
    def _():
        out_ref[0:size16, :] = jnp.zeros((size16, dim), F)

        def zero_copy(c):
            n = tail if c == groups else size16
            return pltpu.make_async_copy(out_ref.at[pl.ds(0, n)], emb_out.at[pl.ds(c * size16, n)], o_sem.at[c])

        for c in range(groups + 1):
            zero_copy(c).start()
        w1_out[...] = w1_in[...]
        b1_out[...] = b1_in[...]
        w2_out[...] = w2_in[...]
        part_out[...] = pin_ref[...]
        pieces = functools.partial(dy_piece, cfg, e_ref, log_ref, lab_ref, lse_ref, xh_ref, dyt_ref, part_out)

        @pl.when(stage == helper)
        def _():
            pieces(SPLIT_DY + DY_LATE, full, True)

        @pl.when(stage != helper)
        def _():
            pieces(DY_LATE, SPLIT_DY, False)

        for c in range(groups + 1):
            zero_copy(c).wait()


def sum_kernel(cfg, e_ref, log_ref, lab_ref, lse_ref, xh_ref, pin_ref, sum_out, part_ref, dyt_ref, got, send_sem, recv_sem):
    stages, tps, toks, dim, vocab = cfg
    rank = lax.axis_index('tp')
    stage = lax.axis_index('pp')
    last = stages - 1
    helper = stages - 2
    mids = helper
    bar = pltpu.get_barrier_semaphore()

    def copy_to(to_stage, off, idx):
        slot = (stage - 1) * tps + rank
        return pltpu.make_async_remote_copy(part_ref, got.at[slot], send_sem.at[idx], recv_sem.at[slot], device_id={'pp': to_stage, 'tp': lax.rem(rank + off, tps)}, device_id_type=MESH)

    def arrived(slot):
        return pltpu.make_async_remote_copy(part_ref, got.at[slot], send_sem.at[0], recv_sem.at[slot], device_id={'tp': rank}, device_id_type=MESH)

    def total(at):
        return functools.reduce(jnp.add, [got[at * tps + r] for r in range(tps)])

    @pl.when((stage != 0) & (stage != last))
    def _():
        for to_stage in range(1, 1 + mids):
            for off in range(tps):
                @pl.when((stage != to_stage) | (off != 0))
                def _():
                    pl.semaphore_signal(bar, inc=1, device_id={'pp': to_stage, 'tp': lax.rem(rank + off, tps)}, device_id_type=MESH)
        part_ref[...] = pin_ref[...]
        pieces = functools.partial(dy_piece, cfg, e_ref, log_ref, lab_ref, lse_ref, xh_ref, dyt_ref, part_ref)

        @pl.when(stage == helper)
        def _():
            pieces(SPLIT_DY, SPLIT_DY + DY_LATE, False)

        @pl.when(stage != helper)
        def _():
            pieces(0, DY_LATE, False)
        pl.semaphore_wait(bar, mids * tps - 1)

        @pl.when(stage == helper)
        def _():
            sends = [copy_to(helper, off, off) for off in range(1, tps)]
            for send in sends:
                send.start()
            got[(helper - 1) * tps + rank] = part_ref[...]
            for at in range(helper - 1):
                for r in range(tps):
                    arrived(at * tps + r).wait_recv()
            for off in range(1, tps):
                arrived((helper - 1) * tps + lax.rem(rank + off, tps)).wait_recv()
            own = total(helper - 1)
            rest = functools.reduce(jnp.add, [total(at) for at in range(helper)])
            sum_out[...] = jnp.concatenate([own[0:2, :], rest[2:8, :]], axis=0)
            for send in sends:
                send.wait_send()

        @pl.when(stage != helper)
        def _():
            sends = [copy_to(helper, off, tps + off) for off in range(tps)] + [copy_to(stage, off, off) for off in range(1, tps)]
            for send in sends:
                send.start()
            mine = (stage - 1) * tps
            got[mine + rank] = part_ref[...]
            for off in range(1, tps):
                arrived(mine + lax.rem(rank + off, tps)).wait_recv()
            sum_out[...] = functools.reduce(jnp.add, [got[mine + r] for r in range(tps)])
            for send in sends:
                send.wait_send()

    @pl.when((stage == 0) | (stage == last))
    def _():
        sum_out[...] = pin_ref[...]


def hand_kernel(cfg, sum_ref, vec_out, got, send_sem, recv_sem):
    stages, tps, toks, dim, vocab = cfg
    stage = lax.axis_index('pp')
    last = stages - 1
    helper = stages - 2
    bar = pltpu.get_barrier_semaphore()

    def hand_over():
        return pltpu.make_async_remote_copy(sum_ref, got, send_sem, recv_sem, device_id={'pp': last}, device_id_type=MESH)

    @pl.when(stage == helper)
    def _():
        pl.semaphore_signal(bar, inc=1, device_id={'pp': last}, device_id_type=MESH)
        pl.semaphore_wait(bar, 1)
        hand_over().start()
        hand_over().wait_send()

    @pl.when(stage != last)
    def _():
        vec_out[0:2, :] = sum_ref[0:2, :]
        vec_out[2:3, :] = jnp.zeros((1, LANES), F)

    @pl.when(stage == last)
    def _():
        pl.semaphore_signal(bar, inc=1, device_id={'pp': helper}, device_id_type=MESH)
        pl.semaphore_wait(bar, 1)
        hand_over().wait_recv()
        vec_out[0:2, :] = got[2:4, :]
        vec_out[2:3, :] = got[4:5, :] * (-1.0 / toks)


def write_kernel(vec_ref, gam_out, bet_out, loss_out):
    gam_out[...] = vec_ref[0:1, :]
    bet_out[...] = vec_ref[1:2, :]
    loss_out[0] = jnp.sum(vec_ref[2:3, :])


def solution(mesh):
    stages, tps = mesh.shape['pp'], mesh.shape['tp']
    lead = ('dp', 'pp')
    hbm = pl.BlockSpec(memory_space=pltpu.HBM)
    vmem = pl.BlockSpec(memory_space=pltpu.VMEM)
    S = jax.ShapeDtypeStruct
    V = pltpu.VMEM
    DMA = pltpu.SemaphoreType.DMA
    I = jnp.int32

    def stay(*arrays):
        return [pltpu.with_memory_space_constraint(a, pltpu.HBM) for a in arrays]

    def body(tok_ids, hid_in, cot_in, ln_gamma, ln_beta, emb_table, w_in, b_in, w_out):
        dim = hid_in.shape[-1]
        hid = hid_in.reshape(-1, dim)
        cot = cot_in.reshape(-1, dim)
        toks = hid.shape[0]
        chunks = toks // LANES
        ids = tok_ids.reshape(chunks, LANES)
        table = emb_table[0]
        vocab = table.shape[0]
        ff = w_in.shape[2]
        cfg = (stages, tps, toks, dim, vocab)
        rows = toks + 2 * chunks
        vec = S((8, LANES), F)
        weights = (S((dim, ff), F), S((1, ff), F), S((ff, dim), F))
        mids = pl.pallas_call(
            functools.partial(stats_kernel, cfg), name='stats',
            out_shape=(S((vocab, dim), B), S((vocab, toks), F), S((vocab, dim), F), S((toks, dim), B), S((8, LANES), I), vec, S((toks, dim), B), S((8, LANES), I), S((toks, dim), F), vec) + weights,
            in_specs=[hbm] * 9, out_specs=[vmem] * 13,
            scratch_shapes=[
                V((chunks, LANES), I), V((toks, dim), B), V((toks, dim), B), V((1, dim), F), V((1, dim), F), V((dim, ff), B), V((1, ff), F), V((ff, dim), B), pltpu.SMEM((chunks, LANES), I),
                V((dim, toks), B), V((2, TILE + 32, toks), F), V((rows, dim), F), V((rows, dim), F), V((rows, dim), F), V((rows, dim), F),
                V((8, LANES), F), V((2 * tps, 8, LANES), F), V((vocab, dim), F), V((toks, dim), F), V((8, LANES), F), V((tps, 8, LANES), F),
                DMA((PARTS,)), DMA((9,)), DMA((4 + stages * tps,)), DMA((2,)), DMA, DMA((2 * tps,)), DMA((tps,))],
            compiler_params=pltpu.CompilerParams(collective_id=0, has_side_effects=True, vmem_limit_bytes=GRANT),
        )(*stay(ids, hid, cot, ln_gamma, ln_beta, table, w_in[0], b_in, w_out[0]))
        groups = (vocab // TILE - 1) // 16 + 1
        emb_grad, w1g, b1g, w2g, part = pl.pallas_call(
            functools.partial(grad_kernel, cfg), name='grads',
            out_shape=(S((vocab, dim), F),) + weights + (vec,),
            in_specs=[vmem] * 13, out_specs=[hbm] + [vmem] * 4,
            scratch_shapes=[V((vocab, dim), F), V((dim, toks), F), DMA((groups,))],
            compiler_params=pltpu.CompilerParams(vmem_limit_bytes=GRANT),
        )(*mids)
        sums = pl.pallas_call(
            functools.partial(sum_kernel, cfg), name='sums', out_shape=vec, in_specs=[vmem] * 6, out_specs=vmem,
            scratch_shapes=[V((8, LANES), F), V((dim, toks), F), V(((stages - 2) * tps, 8, LANES), F), DMA((2 * tps,)), DMA(((stages - 2) * tps,))],
            compiler_params=pltpu.CompilerParams(collective_id=1, has_side_effects=True, vmem_limit_bytes=GRANT),
        )(mids[0], mids[1], mids[4], mids[5], mids[8], part)
        vecs = pl.pallas_call(
            functools.partial(hand_kernel, cfg), name='hand', out_shape=vec, in_specs=[vmem], out_specs=vmem,
            scratch_shapes=[V((8, LANES), F), DMA, DMA],
            compiler_params=pltpu.CompilerParams(collective_id=2, has_side_effects=True, vmem_limit_bytes=4 << 20),
        )(sums)
        gam, bet, loss = pl.pallas_call(
            write_kernel, name='write', out_shape=(S((1, dim), F), S((1, dim), F), S((1,), F)), in_specs=[vmem], out_specs=[vmem] * 2 + [pl.BlockSpec(memory_space=pltpu.SMEM)],
            compiler_params=pltpu.CompilerParams(vmem_limit_bytes=4 << 20),
        )(vecs)
        return emb_grad[None], loss, gam, bet, w1g[None], b1g, w2g[None]

    specs_in = (P(lead, None, None), P(lead, None, None, None), P(lead, None, None, None), P(lead, None), P(lead, None), P(lead, 'tp', None), P(lead, None, 'tp'), P(lead, 'tp'), P(lead, 'tp', None))
    specs_out = (P(lead, 'tp', None), P(lead), P(lead, None), P(lead, None), P(lead, None, 'tp'), P(lead, 'tp'), P(lead, 'tp', None))
    return jax.shard_map(body, mesh=mesh, in_specs=specs_in, out_specs=specs_out, check_vma=False)
```

```python
import functools

import jax
import jax.numpy as jnp
from jax import lax
from jax.experimental import pallas as pl
from jax.experimental.pallas import tpu as pltpu
from jax.sharding import PartitionSpec as P

F = jnp.float32
B = jnp.bfloat16
LN_EPS = 1e-5
LOG2E = 1.4426950408889634
LANES = 128
TILE = 256
SPLIT_STATS = 37
SPLIT_DY = 16
EARLY = 8
FIRST = 16
FRESH = 48
PARTS = 4
LATE_HELPER = 16
LATE_FIRST = 6
GRANT = 14 << 20
MESH = pl.DeviceIdType.MESH
NT = (((1,), (1,)), ((), ()))
TN = (((0,), (0,)), ((), ()))


def ln_hat(rows):
    centre = rows - jnp.mean(rows, axis=-1, keepdims=True)
    inv = lax.rsqrt(jnp.mean(centre * centre, axis=-1, keepdims=True) + LN_EPS)
    return centre * inv, inv


def tile_ids(row, size):
    return (lax.broadcasted_iota(jnp.int32, (size, LANES), 0) + row).astype(jnp.int16)


def local_ids(ref, chunks, base, vocab):
    ids = lanes_row(ref, 0, chunks) - base
    return jnp.where((ids >= 0) & (ids < vocab), ids, -1).astype(jnp.int16)


def steps(count):
    return max(d for d in range(1, 14) if count % d == 0)


def mm(a, b):
    return jnp.dot(a, b, preferred_element_type=F)


def lanes_row(ref, first, chunks):
    return jnp.concatenate([ref[first + c:first + c + 1, :] for c in range(chunks)], axis=1)


def stats_kernel(cfg, ids_hbm, hid_hbm, cot_hbm, gam_hbm, bet_hbm, emb_hbm, w1_hbm, b1_hbm, w2_hbm,
                 e_ref, log_ref, first_ref, y_out, lab_out, lse_out, dx_out, did_out, xh_out, part_out, w1_out, w2_out, yt_ref,
                 ids_ref, hid_ref, cot_ref, gam_ref, bet_ref, w1_ref, b1_ref, w2_ref, ids_smem,
                 buf, pack_src, pack_dst, dx_src, dx_dst, st_src, st_all, e32_ref, x_ref, part_src, part_all,
                 e_sem, in_sem, send_sem, many_sem, pack_sem, dx_sem, st_sem, part_sem):
    stages, tps, toks, dim, vocab = cfg
    chunks = toks // LANES
    rank = lax.axis_index('tp')
    stage = lax.axis_index('pp')
    last = stages - 1
    helper = stages - 2
    full, tail = vocab // TILE - 1, vocab - (vocab // TILE - 1) * TILE
    vecs = 2 * chunks
    half = toks // 2
    cuts = [i * (full // PARTS) for i in range(PARTS)] + [full]

    def e_part(i):
        start = cuts[i] * TILE
        size = (vocab if i == PARTS - 1 else cuts[i + 1] * TILE) - start
        return pltpu.make_async_copy(emb_hbm.at[pl.ds(start, size)], e_ref.at[pl.ds(start, size)], e_sem.at[i])

    e_parts = [e_part(i) for i in range(PARTS)]
    pairs = ((hid_hbm, hid_ref), (ids_hbm, ids_ref), (gam_hbm, gam_ref), (bet_hbm, bet_ref), (cot_hbm, cot_ref), (ids_hbm, ids_smem), (w1_hbm, w1_ref), (b1_hbm, b1_ref), (w2_hbm, w2_ref))
    hid_ld, ids_ld, gam_ld, bet_ld, cot_ld, smem_ld, w1_ld, b1_ld, w2_ld = [pltpu.make_async_copy(a, b, in_sem.at[i]) for i, (a, b) in enumerate(pairs)]

    def fetch(*copies):
        for copy in copies:
            copy.start()

    def ready(*copies):
        for copy in copies:
            copy.wait()

    def remote(src, dst, ssem, rsem, to_stage, off=0):
        return pltpu.make_async_remote_copy(src, dst, ssem, rsem, device_id={'pp': to_stage, 'tp': lax.rem(rank + off, tps)}, device_id_type=MESH)

    def pack_rows(which):
        return pl.ds(0, vecs + half) if which == 0 else pl.ds(vecs + half, half)

    def pack_copy(to_stage, which, idx, src):
        return remote(src.at[pack_rows(which)], pack_dst.at[pack_rows(which)], send_sem.at[idx], pack_sem.at[which], to_stage)

    def pack_sends():
        return [pack_copy(helper, 0, 0, pack_src), pack_copy(helper, 1, 1, pack_src), pack_copy(0, 0, 2, pack_src), pack_copy(0, 1, 3, pack_src)]

    def relays():
        return [pack_copy(1, w, 1 + w, pack_dst) for w in range(2)]

    def dx_copy():
        return remote(dx_src, dx_dst, send_sem.at[0], dx_sem, last)

    def part_copy(off):
        return remote(part_src, part_all.at[rank], many_sem, part_sem, 0, off)

    def greet():
        bar = pltpu.get_barrier_semaphore()
        for ds in range(stages):
            for off in range(tps):
                if ds or off:
                    pl.semaphore_signal(bar, inc=1, device_id={'pp': lax.rem(stage + ds, stages), 'tp': lax.rem(rank + off, tps)}, device_id_type=MESH)

    def met():
        pl.semaphore_wait(pltpu.get_barrier_semaphore(), stages * tps - 1)

    def normed(rows, gam, bet, start, size):
        hat, _ = ln_hat(rows)
        norm = (hat * gam + bet).astype(B)
        xh_out[start:start + size, :] = hat
        y_out[start:start + size, :] = norm
        yt_ref[:, start:start + size] = norm.astype(F).T.astype(B)

    def unpack(which):
        start = which * half
        normed(pack_dst[vecs + start:vecs + start + half, :], pack_dst[chunks:chunks + 1, :], pack_dst[chunks + 1:chunks + 2, :], start, half)
        if which == 0:
            lab_out[0:chunks, :] = pack_dst[0:chunks, :].astype(jnp.int32)

    def unpack_all():
        for w in range(2):
            pack_copy(helper, w, 0, pack_src).wait_recv()
            unpack(w)

    def st_sends(which):
        slot = 2 * rank + which
        return [remote(st_src, st_all.at[slot], many_sem, st_sem, lax.rem(stage + ds, stages), off) for ds in range(stages) for off in range(tps) if ds or off]

    def st_wait(count):
        got = st_all.at[pl.ds(0, count)]
        remote(got, got, many_sem, st_sem, last).wait_recv()

    def st_sent():
        sent = pack_src.at[pl.ds(0, 8 * (stages * tps - 1))]
        remote(sent, sent, many_sem, st_sem, last).wait_send()

    def finish_stats():
        tops = [st_all[r, 0:chunks, :] for r in range(2 * tps)]
        sums = [st_all[r, chunks:2 * chunks, :] for r in range(2 * tps)]
        top = functools.reduce(jnp.maximum, tops)
        tot = functools.reduce(jnp.add, [s * jnp.exp(t - top) for s, t in zip(sums, tops)])
        lse_out[0:chunks, :] = top + jnp.log(tot)

    def logit_tile(row, size):
        logits = mm(e_ref[pl.ds(row, size), :], yt_ref[...])
        log_ref[pl.ds(row, size), :] = logits
        return logits

    def fill_logits(first, end):
        def step(i, carry):
            logit_tile(pl.multiple_of(i * TILE, TILE), TILE)
            return carry
        lax.fori_loop(first, end, step, 0, unroll=steps(end - first))

    def first_tiles(first, end):
        did = local_ids(did_out, chunks, rank * vocab, vocab)

        def fill(row, size):
            rows = tile_ids(row, size)
            one, zero = jnp.ones((size, LANES), B), jnp.zeros((size, LANES), B)
            h = [jnp.where(rows == did[:, c * LANES:(c + 1) * LANES], one, zero) for c in range(chunks)]
            first_ref[pl.ds(row, size), :] = mm(jnp.concatenate(h, axis=1), dx_out[...])

        def step(i, carry):
            fill(pl.multiple_of(i * TILE, TILE), TILE)
            return carry
        lax.fori_loop(first, end, step, 0, unroll=steps(end - first))
        if end == full:
            fill(full * TILE, tail)

    def logits_to(row, slot, top, size=TILE):
        logits = logit_tile(row, size)
        buf[slot, 0:size] = logits
        return jnp.maximum(top, jnp.max(logits.reshape(size // 8, 8, toks), axis=0))

    def add_exp(slot, top_old, top, tot, size=TILE):
        ex = jnp.exp(buf[slot, 0:size].reshape(size // 8, 8, toks) - top[None])
        return tot * jnp.exp(top_old - top) + jnp.sum(ex, axis=0)

    def begin_stats(first):
        low = jnp.full((8, toks), -jnp.inf, F)
        top = logits_to(first * TILE, 0, low)
        return top, top, jnp.zeros((8, toks), F)

    def run_stats(first, pairs, carry):
        def step(i, carry):
            old, top, tot = carry
            row = pl.multiple_of(first * TILE + i * 2 * TILE, TILE)
            mid = logits_to(row + TILE, 1, top)
            tot = add_exp(0, old, top, tot)
            new = logits_to(row + 2 * TILE, 0, mid)
            tot = add_exp(1, top, mid, tot)
            return mid, new, tot
        return lax.fori_loop(0, pairs, step, carry, unroll=steps(pairs))

    def share_stats(top, tot, which):
        high = jnp.max(top, axis=0, keepdims=True)
        tot = jnp.sum(tot * jnp.exp(top - high), axis=0, keepdims=True)
        for c in range(chunks):
            st_src[c:c + 1, :] = high[:, c * LANES:(c + 1) * LANES]
            st_src[chunks + c:chunks + c + 1, :] = tot[:, c * LANES:(c + 1) * LANES]
        st_all[2 * rank + which] = st_src[...]
        for send in st_sends(which):
            send.start()

    def mlp():
        ready(hid_ld, cot_ld, gam_ld, bet_ld, w1_ld, b1_ld, w2_ld)
        hat, _ = ln_hat(hid_ref[...].astype(F))
        norm = (hat * gam_ref[...] + bet_ref[...]).astype(B)
        pre = mm(norm, w1_ref[...]) + b1_ref[...]
        cube = 0.7978845608028654 * (pre + 0.044715 * (pre * pre * pre))
        th = jnp.tanh(cube)
        act = pre * (0.5 * (1.0 + th))
        slope = 0.5 * (1.0 + th) + pre * (0.5 * (1.0 - th * th)) * (0.7978845608028654 * (1.0 + 3 * 0.044715 * pre * pre))
        w2_out[...] = lax.dot_general(act.astype(B), cot_ref[...], TN, preferred_element_type=F)
        d_act = lax.dot_general(cot_ref[...], w2_ref[...], NT, preferred_element_type=F)
        d_pre = d_act * slope
        d_b = d_pre.astype(B)
        w1_out[...] = lax.dot_general(norm, d_b, TN, preferred_element_type=F)
        part_out[5:6, :] = jnp.sum(d_pre, axis=0, keepdims=True)
        d_h = lax.dot_general(d_b, w1_ref[...], NT, preferred_element_type=F)
        part_out[0:1, :] = jnp.sum(d_h * hat, axis=0, keepdims=True)
        part_out[1:2, :] = jnp.sum(d_h, axis=0, keepdims=True)
        part_out[2:5, :] = jnp.zeros((3, LANES), F)
        part_out[6:8, :] = jnp.zeros((2, LANES), F)

    @pl.when(stage == last)
    def _():
        fetch(hid_ld, ids_ld, gam_ld, bet_ld, e_parts[0])
        greet()
        ready(hid_ld, ids_ld, gam_ld, bet_ld)
        fetch(*e_parts[1:])
        rows = hid_ref[...].astype(F)
        pack_src[vecs:vecs + toks, :] = rows
        pack_src[0:chunks, :] = ids_ref[...].astype(F)
        pack_src[chunks:chunks + 1, :] = gam_ref[...]
        pack_src[chunks + 1:chunks + 2, :] = bet_ref[...]
        pack_src[chunks + 2:vecs, :] = jnp.zeros((vecs - chunks - 2, dim), F)
        normed(rows, gam_ref[...], bet_ref[...], 0, toks)
        lab_out[0:chunks, :] = ids_ref[...]
        e_parts[0].wait()
        carry = run_stats(0, EARLY // 2, begin_stats(0))
        met()
        packs = pack_sends()
        for send in packs:
            send.start()
        ready(*e_parts[1:])
        old, top, tot = run_stats(EARLY, (SPLIT_STATS - 1 - EARLY) // 2, carry)
        tot = add_exp(0, old, top, tot)
        share_stats(top, tot, 0)
        fill_logits(SPLIT_STATS, full)
        logit_tile(full * TILE, tail)
        dx_copy().wait_recv()
        dx_out[...] = dx_dst[0:toks, :].astype(B)
        did_out[0:chunks, :] = dx_dst[toks:toks + chunks, :].astype(jnp.int32)
        first_tiles(0, FIRST)
        st_wait(2 * tps - 1)
        finish_stats()
        for send in packs:
            send.wait_send()
        st_sent()

    @pl.when(stage == helper)
    def _():
        fetch(hid_ld, cot_ld, gam_ld, bet_ld, w1_ld, b1_ld, w2_ld, *e_parts)
        greet()
        mlp()
        met()
        ready(*e_parts)
        unpack_all()
        old, top, tot = run_stats(SPLIT_STATS, (full - 1 - SPLIT_STATS) // 2, begin_stats(SPLIT_STATS))
        new = logits_to(full * TILE, 1, top, tail)
        tot = add_exp(0, old, top, tot)
        tot = add_exp(1, top, new, tot, tail)
        share_stats(new, tot, 1)
        fill_logits(SPLIT_DY, SPLIT_STATS)
        st_wait(2 * tps - 1)
        finish_stats()
        st_sent()

    @pl.when(stage == 0)
    def _():
        fetch(cot_ld, ids_ld, gam_ld, smem_ld, *e_parts)
        greet()
        ready(cot_ld, ids_ld, gam_ld, smem_ld)

        def widen(i, carry):
            row = pl.multiple_of(i * TILE, TILE)
            e32_ref[pl.ds(row, TILE), :] = e_ref[pl.ds(row, TILE), :].astype(F)
            return carry

        for i in range(PARTS):
            e_parts[i].wait()
            lax.fori_loop(cuts[i], cuts[i + 1], widen, 0, unroll=4)
        e32_ref[full * TILE:vocab, :] = e_ref[full * TILE:vocab, :].astype(F)
        base = rank * vocab
        for c in range(chunks):
            def pick(i, carry):
                row = jnp.clip(ids_smem[c, i] - base, 0, vocab - 1)
                x_ref[pl.ds(c * LANES + i, 1), :] = e32_ref[pl.ds(row, 1), :]
                return carry
            lax.fori_loop(0, LANES, pick, 0, unroll=16)
        local = lanes_row(ids_ref, 0, chunks) - base
        inside = jnp.where((local >= 0) & (local < vocab), 1.0, 0.0)
        mask = jnp.broadcast_to(inside, (LANES, toks)).T
        hat, inv = ln_hat(x_ref[...])
        cot = cot_ref[...].astype(F)
        scaled = cot * gam_ref[...]
        grad = inv * (scaled - jnp.mean(scaled, axis=-1, keepdims=True) - hat * jnp.mean(scaled * hat, axis=-1, keepdims=True))
        grad = jnp.where(mask > 0.5, grad, 0.0).astype(B)
        dx_out[...] = grad
        did_out[0:chunks, :] = ids_ref[...]
        dx_src[0:toks, :] = grad.astype(F)
        dx_src[toks:toks + chunks, :] = ids_ref[...].astype(F)
        part_src[0:1, :] = jnp.sum(jnp.where(mask > 0.5, cot * hat, 0.0), axis=0, keepdims=True)
        part_src[1:2, :] = jnp.sum(jnp.where(mask > 0.5, cot, 0.0), axis=0, keepdims=True)
        part_src[2:8, :] = jnp.zeros((6, LANES), F)
        part_all[rank] = part_src[...]
        met()
        dx_copy().start()
        for off in range(1, tps):
            part_copy(off).start()
        first_tiles(0, full)
        sends = relays()
        for w in range(2):
            pack_copy(0, w, 0, pack_src).wait_recv()
            sends[w].start()
            unpack(w)
        fill_logits(0, full)
        logit_tile(full * TILE, tail)
        others = part_all.at[pl.ds(0, tps - 1)]
        remote(others, others, many_sem, part_sem, 0, 1).wait_recv()
        part_out[...] = functools.reduce(jnp.add, [part_all[r] for r in range(tps)])
        st_wait(2 * tps)
        finish_stats()
        dx_copy().wait_send()
        for send in sends:
            send.wait_send()
        remote(others, others, many_sem, part_sem, 0, 1).wait_send()

    @pl.when((stage != 0) & (stage != helper) & (stage != last))
    def _():
        fetch(hid_ld, cot_ld, gam_ld, bet_ld, w1_ld, b1_ld, w2_ld, *e_parts)
        greet()
        mlp()
        met()
        ready(*e_parts)
        unpack_all()
        fill_logits(0, SPLIT_DY)
        st_wait(2 * tps)
        finish_stats()


def dy_piece(cfg, e_ref, log_ref, lab_ref, lse_ref, xh_ref, dyt_ref, part_ref, first, end, with_tail):
    stages, tps, toks, dim, vocab = cfg
    chunks = toks // LANES
    full, tail = vocab // TILE - 1, vocab - (vocab // TILE - 1) * TILE
    lse = lanes_row(lse_ref, 0, chunks)
    lab = lanes_row(lab_ref, 0, chunks) - lax.axis_index('tp') * vocab
    dyt_ref[...] = jnp.zeros((dim, toks), F)

    def work(row, size, seen):
        x = log_ref[pl.ds(row, size), :] - lse
        p = jnp.exp2(x * LOG2E)
        rows = lax.broadcasted_iota(jnp.int32, (size, LANES), 0) + row
        g, found = [], []
        for c in range(chunks):
            cols = slice(c * LANES, (c + 1) * LANES)
            hit = rows == lab[:, cols]
            pc, xc, at = p[:, cols], x[:, cols], seen[c]
            g.append(jnp.where(hit, pc - 1.0, pc).astype(B))
            for k in range(0, size, 8):
                at = jnp.where(hit[k:k + 8, :], xc[k:k + 8, :], at)
            found.append(at)
        dyt_ref[...] += lax.dot_general(e_ref[pl.ds(row, size), :], jnp.concatenate(g, axis=1), TN, preferred_element_type=F)
        return tuple(found)

    def step(i, seen):
        return work(pl.multiple_of(i * TILE, TILE), TILE, seen)

    seen = lax.fori_loop(first, end, step, tuple(jnp.zeros((8, LANES), F) for _ in range(chunks)), unroll=steps(end - first))
    if with_tail:
        seen = work(full * TILE, tail, seen)
    loss = functools.reduce(jnp.add, seen)
    dy = dyt_ref[...].T
    part_ref[2:3, :] += jnp.sum(dy * xh_ref[...], axis=0, keepdims=True)
    part_ref[3:4, :] += jnp.sum(dy, axis=0, keepdims=True)
    part_ref[4:5, :] += jnp.sum(loss, axis=0, keepdims=True)


def grad_kernel(cfg, e_ref, log_ref, first_ref, y_ref, lab_ref, lse_ref, dx_ref, did_ref, xh_ref, pin_ref, w1_in, w2_in, yt_ref,
                emb_out, w1_out, b1_out, w2_out, part_out, out_ref, dyt_ref, zero_ref, bias_ref, o_sem, w_sem):
    stages, tps, toks, dim, vocab = cfg
    chunks = toks // LANES
    rank = lax.axis_index('tp')
    stage = lax.axis_index('pp')
    last = stages - 1
    helper = stages - 2
    base = rank * vocab
    full, tail = vocab // TILE - 1, vocab - (vocab // TILE - 1) * TILE
    bounds = (0, 16, 32, 44, full)
    spans = [(bounds[i], bounds[i + 1]) for i in range(4)]
    size16 = 16 * TILE

    def small(w1_src, w2_src):
        return [pltpu.make_async_copy(w1_src, w1_out, w_sem.at[0]), pltpu.make_async_copy(bias_ref, b1_out, w_sem.at[1]), pltpu.make_async_copy(w2_src, w2_out, w_sem.at[2])]

    @pl.when((stage == 0) | (stage == last))
    def _():
        zero_ref[...] = jnp.zeros(zero_ref.shape, F)
        bias_ref[...] = jnp.zeros(bias_ref.shape, F)
        smalls = small(zero_ref, zero_ref)
        for copy in smalls:
            copy.start()
        part_out[...] = pin_ref[...]
        lse = lanes_row(lse_ref, 0, chunks)
        lab = local_ids(lab_ref, chunks, base, vocab)
        did = local_ids(did_ref, chunks, base, vocab)

        def out_copy(c):
            start, size = (full * TILE, tail) if c == len(spans) else (spans[c][0] * TILE, (spans[c][1] - spans[c][0]) * TILE)
            return pltpu.make_async_copy(out_ref.at[pl.ds(start, size)], emb_out.at[pl.ds(start, size)], o_sem.at[c])

        def work(row, size, pick, fresh):
            logits = mm(e_ref[pl.ds(row, size), :], yt_ref[...]) if fresh else log_ref[pl.ds(row, size), :]
            p = jnp.exp2((logits - lse) * LOG2E)
            rows = tile_ids(row, size)
            one, zero = jnp.ones((size, LANES), B), jnp.zeros((size, LANES), B)
            g, h = [], []
            for c in range(chunks):
                cols = slice(c * LANES, (c + 1) * LANES)
                pc = p[:, cols]
                g.append(jnp.where(rows == lab[:, cols], (pc - 1.0).astype(B), pc.astype(B)))
                if pick:
                    h.append(jnp.where(rows == did[:, cols], one, zero))
            first = mm(jnp.concatenate(h, axis=1), dx_ref[...]) if pick else first_ref[pl.ds(row, size), :]
            out_ref[pl.ds(row, size), :] = first + mm(jnp.concatenate(g, axis=1), y_ref[...])

        def sweep(first, end, pick, fresh=False):
            def step(i, carry):
                work(pl.multiple_of(i * TILE, TILE), TILE, pick, fresh)
                return carry
            lax.fori_loop(first, end, step, 0, unroll=min(16, end - first))

        def both(run, fresh):
            pl.when(stage == 0)(lambda: run(False, fresh))
            pl.when(stage != 0)(lambda: run(True, False))

        both(lambda pick, fresh: work(full * TILE, tail, pick, fresh), False)
        out_copy(len(spans)).start()
        for c, (first, end) in enumerate(spans):
            if end <= FIRST:
                sweep(first, end, False)
            else:
                both(functools.partial(sweep, first, end), first >= FRESH)
            out_copy(c).start()
        for c in range(len(spans) + 1):
            out_copy(c).wait()
        for copy in smalls:
            copy.wait()

    @pl.when((stage != 0) & (stage != last))
    def _():
        out_ref[0:size16, :] = jnp.zeros((size16, dim), F)

        bias_ref[...] = pin_ref[5:6, :]
        zeros = [pltpu.make_async_copy(out_ref.at[pl.ds(0, n)], emb_out.at[pl.ds(c * size16, n)], o_sem.at[c]) for c, n in enumerate((size16, size16, size16, tail))]
        smalls = small(w1_in, w2_in)
        for copy in zeros + smalls:
            copy.start()
        part_out[...] = pin_ref[...]
        pieces = functools.partial(dy_piece, cfg, e_ref, log_ref, lab_ref, lse_ref, xh_ref, dyt_ref, part_out)

        @pl.when(stage == helper)
        def _():
            pieces(SPLIT_DY + LATE_HELPER, full, True)

        @pl.when(stage != helper)
        def _():
            pieces(LATE_FIRST, SPLIT_DY, False)

        for copy in zeros + smalls:
            copy.wait()


def sum_kernel(cfg, e_ref, log_ref, lab_ref, lse_ref, xh_ref, pin_ref, sum_out, part_ref, dyt_ref, got, send_sem, recv_sem):
    stages, tps, toks, dim, vocab = cfg
    rank = lax.axis_index('tp')
    stage = lax.axis_index('pp')
    last = stages - 1
    helper = stages - 2
    mids = helper
    bar = pltpu.get_barrier_semaphore()

    def copy_to(to_stage, off):
        slot = (stage - 1) * tps + rank
        return pltpu.make_async_remote_copy(part_ref, got.at[slot], send_sem, recv_sem, device_id={'pp': to_stage, 'tp': lax.rem(rank + off, tps)}, device_id_type=MESH)

    def batch(count):
        some = got.at[pl.ds(0, count)]
        return pltpu.make_async_remote_copy(some, some, send_sem, recv_sem, device_id={'tp': lax.rem(rank + 1, tps)}, device_id_type=MESH)

    def total(at):
        return functools.reduce(jnp.add, [got[at * tps + r] for r in range(tps)])

    @pl.when((stage != 0) & (stage != last))
    def _():
        for to_stage in range(1, 1 + mids):
            for off in range(tps):
                @pl.when((stage != to_stage) | (off != 0))
                def _():
                    pl.semaphore_signal(bar, inc=1, device_id={'pp': to_stage, 'tp': lax.rem(rank + off, tps)}, device_id_type=MESH)
        part_ref[...] = pin_ref[...]
        pieces = functools.partial(dy_piece, cfg, e_ref, log_ref, lab_ref, lse_ref, xh_ref, dyt_ref, part_ref)

        @pl.when(stage == helper)
        def _():
            pieces(SPLIT_DY, SPLIT_DY + LATE_HELPER, False)

        @pl.when(stage != helper)
        def _():
            pieces(0, LATE_FIRST, False)
        pl.semaphore_wait(bar, mids * tps - 1)

        @pl.when(stage == helper)
        def _():
            sends = [copy_to(helper, off) for off in range(1, tps)]
            for send in sends:
                send.start()
            got[(helper - 1) * tps + rank] = part_ref[...]
            batch(mids * tps - 1).wait_recv()
            own = total(helper - 1)
            rest = functools.reduce(jnp.add, [total(at) for at in range(helper)])
            sum_out[...] = jnp.concatenate([own[0:2, :], rest[2:8, :]], axis=0)
            batch(tps - 1).wait_send()

        @pl.when(stage != helper)
        def _():
            sends = [copy_to(helper, off) for off in range(tps)] + [copy_to(stage, off) for off in range(1, tps)]
            for send in sends:
                send.start()
            mine = (stage - 1) * tps
            got[mine + rank] = part_ref[...]
            batch(tps - 1).wait_recv()
            sum_out[...] = functools.reduce(jnp.add, [got[mine + r] for r in range(tps)])
            batch(2 * tps - 1).wait_send()

    @pl.when((stage == 0) | (stage == last))
    def _():
        sum_out[...] = pin_ref[...]


def hand_kernel(cfg, sum_ref, vec_out, got, send_sem, recv_sem):
    stages, tps, toks, dim, vocab = cfg
    stage = lax.axis_index('pp')
    last = stages - 1
    helper = stages - 2
    bar = pltpu.get_barrier_semaphore()

    def hand_over():
        return pltpu.make_async_remote_copy(sum_ref, got, send_sem, recv_sem, device_id={'pp': last}, device_id_type=MESH)

    @pl.when(stage == helper)
    def _():
        pl.semaphore_signal(bar, inc=1, device_id={'pp': last}, device_id_type=MESH)
        pl.semaphore_wait(bar, 1)
        hand_over().start()
        hand_over().wait_send()

    @pl.when(stage != last)
    def _():
        vec_out[0:2, :] = sum_ref[0:2, :]
        vec_out[2:3, :] = jnp.zeros((1, LANES), F)

    @pl.when(stage == last)
    def _():
        pl.semaphore_signal(bar, inc=1, device_id={'pp': helper}, device_id_type=MESH)
        pl.semaphore_wait(bar, 1)
        hand_over().wait_recv()
        vec_out[0:2, :] = got[2:4, :]
        vec_out[2:3, :] = got[4:5, :] * (-1.0 / toks)


def write_kernel(vec_ref, gam_out, bet_out, loss_out):
    gam_out[...] = vec_ref[0:1, :]
    bet_out[...] = vec_ref[1:2, :]
    loss_out[0] = jnp.sum(vec_ref[2:3, :])


def solution(mesh):
    stages, tps = mesh.shape['pp'], mesh.shape['tp']
    lead = ('dp', 'pp')
    hbm = pl.BlockSpec(memory_space=pltpu.HBM)
    vmem = pl.BlockSpec(memory_space=pltpu.VMEM)
    S = jax.ShapeDtypeStruct
    V = pltpu.VMEM
    DMA = pltpu.SemaphoreType.DMA
    I = jnp.int32

    def stay(*arrays):
        return [pltpu.with_memory_space_constraint(a, pltpu.HBM) for a in arrays]

    def body(tok_ids, hid_in, cot_in, ln_gamma, ln_beta, emb_table, w_in, b_in, w_out):
        dim = hid_in.shape[-1]
        hid = hid_in.reshape(-1, dim)
        cot = cot_in.reshape(-1, dim)
        toks = hid.shape[0]
        chunks = toks // LANES
        ids = tok_ids.reshape(chunks, LANES)
        table = emb_table[0]
        vocab = table.shape[0]
        ff = w_in.shape[2]
        cfg = (stages, tps, toks, dim, vocab)
        rows = toks + 2 * chunks
        vec = S((8, LANES), F)
        weights = (S((dim, ff), F), S((ff, dim), F))
        mids = pl.pallas_call(
            functools.partial(stats_kernel, cfg), name='stats',
            out_shape=(S((vocab, dim), B), S((vocab, toks), F), S((vocab, dim), F), S((toks, dim), B), S((8, LANES), I), vec, S((toks, dim), B), S((8, LANES), I), S((toks, dim), F), vec) + weights + (S((dim, toks), B),),
            in_specs=[hbm] * 9, out_specs=[vmem] * 13,
            scratch_shapes=[
                V((chunks, LANES), I), V((toks, dim), B), V((toks, dim), B), V((1, dim), F), V((1, dim), F), V((dim, ff), B), V((1, ff), F), V((ff, dim), B), pltpu.SMEM((chunks, LANES), I),
                V((2, TILE + 32, toks), F), V((rows, dim), F), V((rows, dim), F), V((rows, dim), F), V((rows, dim), F),
                V((8, LANES), F), V((2 * tps, 8, LANES), F), V((vocab, dim), F), V((toks, dim), F), V((8, LANES), F), V((tps, 8, LANES), F),
                DMA((PARTS,)), DMA((9,)), DMA((4,)), DMA, DMA((2,)), DMA, DMA, DMA],
            compiler_params=pltpu.CompilerParams(collective_id=0, has_side_effects=True, vmem_limit_bytes=GRANT),
        )(*stay(ids, hid, cot, ln_gamma, ln_beta, table, w_in[0], b_in, w_out[0]))
        emb_grad, w1g, b1g, w2g, part = pl.pallas_call(
            functools.partial(grad_kernel, cfg), name='grads',
            out_shape=(S((vocab, dim), F), S((dim, ff), F), S((1, ff), F), S((ff, dim), F), vec),
            in_specs=[vmem] * 13, out_specs=[hbm] * 4 + [vmem],
            scratch_shapes=[V((vocab, dim), F), V((dim, toks), F), V((dim, ff), F), V((1, ff), F), DMA((5,)), DMA((3,))],
            compiler_params=pltpu.CompilerParams(vmem_limit_bytes=GRANT),
        )(*mids)
        sums = pl.pallas_call(
            functools.partial(sum_kernel, cfg), name='sums', out_shape=vec, in_specs=[vmem] * 6, out_specs=vmem,
            scratch_shapes=[V((8, LANES), F), V((dim, toks), F), V(((stages - 2) * tps, 8, LANES), F), DMA, DMA],
            compiler_params=pltpu.CompilerParams(collective_id=1, has_side_effects=True, vmem_limit_bytes=GRANT),
        )(mids[0], mids[1], mids[4], mids[5], mids[8], part)
        vecs = pl.pallas_call(
            functools.partial(hand_kernel, cfg), name='hand', out_shape=vec, in_specs=[vmem], out_specs=vmem,
            scratch_shapes=[V((8, LANES), F), DMA, DMA],
            compiler_params=pltpu.CompilerParams(collective_id=2, has_side_effects=True, vmem_limit_bytes=4 << 20),
        )(sums)
        gam, bet, loss = pl.pallas_call(
            write_kernel, name='write', out_shape=(S((1, dim), F), S((1, dim), F), S((1,), F)), in_specs=[vmem], out_specs=[vmem] * 2 + [pl.BlockSpec(memory_space=pltpu.SMEM)],
            compiler_params=pltpu.CompilerParams(vmem_limit_bytes=4 << 20),
        )(vecs)
        return emb_grad[None], loss, gam, bet, w1g[None], b1g, w2g[None]

    specs_in = (P(lead, None, None), P(lead, None, None, None), P(lead, None, None, None), P(lead, None), P(lead, None), P(lead, 'tp', None), P(lead, None, 'tp'), P(lead, 'tp'), P(lead, 'tp', None))
    specs_out = (P(lead, 'tp', None), P(lead), P(lead, None), P(lead, None), P(lead, None, 'tp'), P(lead, 'tp'), P(lead, 'tp', None))
    return jax.shard_map(body, mesh=mesh, in_specs=specs_in, out_specs=specs_out, check_vma=False)
```

```python
import functools

import jax
import jax.numpy as jnp
from jax import lax
from jax.experimental import pallas as pl
from jax.experimental.pallas import tpu as pltpu
from jax.sharding import PartitionSpec as P

F = jnp.float32
B = jnp.bfloat16
LN_EPS = 1e-5
LOG2E = 1.4426950408889634
LANES = 128
TILE = 256
SPLIT_STATS = 37
SPLIT_DY = 16
EARLY = 8
FIRST = 16
FRESH = 48
PARTS = 4
LATE_HELPER = 16
LATE_FIRST = 6
GRANT = 14 << 20
MESH = pl.DeviceIdType.MESH
NT = (((1,), (1,)), ((), ()))
TN = (((0,), (0,)), ((), ()))


def col_sum(values):
    return jnp.sum(values, axis=0, keepdims=True)


def row_mean(values):
    return jnp.mean(values, axis=-1, keepdims=True)


def ln_hat(rows):
    centre = rows - row_mean(rows)
    inv = lax.rsqrt(row_mean(centre * centre) + LN_EPS)
    return centre * inv, inv


def tile_ids(row, size):
    return (lax.broadcasted_iota(jnp.int32, (size, LANES), 0) + row).astype(jnp.int16)


def local_ids(ref, chunks, base, vocab):
    ids = lanes_row(ref, 0, chunks) - base
    return jnp.where((ids >= 0) & (ids < vocab), ids, -1).astype(jnp.int16)


def steps(count):
    return max(d for d in range(1, 14) if count % d == 0)


def mm(a, b):
    return jnp.dot(a, b, preferred_element_type=F)


def lanes_row(ref, first, chunks):
    return jnp.concatenate([ref[first + c:first + c + 1, :] for c in range(chunks)], axis=1)


def stats_kernel(cfg, ids_hbm, hid_hbm, cot_hbm, gam_hbm, bet_hbm, emb_hbm, w1_hbm, b1_hbm, w2_hbm,
                 e_ref, log_ref, first_ref, y_out, lab_out, lse_out, dx_out, did_out, xh_out, part_out, w1_out, w2_out, yt_ref, tgt_out,
                 ids_ref, hid_ref, cot_ref, gam_ref, bet_ref, w1_ref, b1_ref, w2_ref, ids_smem,
                 where_ref, where_smem, tgt_src, tgt_dst, buf, pack_src, pack_dst, dx_src, dx_dst, st_src, st_all, e32_ref, x_ref, part_src, part_all,
                 e_sem, in_sem, send_sem, many_sem, pack_sem, dx_sem, st_sem, part_sem, tgt_sem):
    stages, tps, toks, dim, vocab = cfg
    chunks = toks // LANES
    rank = lax.axis_index('tp')
    stage = lax.axis_index('pp')
    last = stages - 1
    helper = stages - 2
    full, tail = vocab // TILE - 1, vocab - (vocab // TILE - 1) * TILE
    vecs = 2 * chunks
    half = toks // 2
    cuts = [i * (full // PARTS) for i in range(PARTS)] + [full]

    def e_part(i):
        start = cuts[i] * TILE
        size = (vocab if i == PARTS - 1 else cuts[i + 1] * TILE) - start
        return pltpu.make_async_copy(emb_hbm.at[pl.ds(start, size)], e_ref.at[pl.ds(start, size)], e_sem.at[i])

    e_parts = [e_part(i) for i in range(PARTS)]
    pairs = ((hid_hbm, hid_ref), (ids_hbm, ids_ref), (gam_hbm, gam_ref), (bet_hbm, bet_ref), (cot_hbm, cot_ref), (ids_hbm, ids_smem), (w1_hbm, w1_ref), (b1_hbm, b1_ref), (w2_hbm, w2_ref))
    hid_ld, ids_ld, gam_ld, bet_ld, cot_ld, smem_ld, w1_ld, b1_ld, w2_ld = [pltpu.make_async_copy(a, b, in_sem.at[i]) for i, (a, b) in enumerate(pairs)]

    def fetch(*copies):
        for copy in copies:
            copy.start()

    def ready(*copies):
        for copy in copies:
            copy.wait()

    def remote(src, dst, ssem, rsem, to_stage, off=0):
        return pltpu.make_async_remote_copy(src, dst, ssem, rsem, device_id={'pp': to_stage, 'tp': lax.rem(rank + off, tps)}, device_id_type=MESH)

    def pack_rows(which):
        return pl.ds(0, vecs + half) if which == 0 else pl.ds(vecs + half, half)

    def pack_copy(to_stage, which, idx, src):
        return remote(src.at[pack_rows(which)], pack_dst.at[pack_rows(which)], send_sem.at[idx], pack_sem.at[which], to_stage)

    def pack_sends():
        return [pack_copy(helper, 0, 0, pack_src), pack_copy(helper, 1, 1, pack_src), pack_copy(0, 0, 2, pack_src), pack_copy(0, 1, 3, pack_src)]

    def relays():
        return [pack_copy(1, w, 1 + w, pack_dst) for w in range(2)]

    def dx_copy():
        return remote(dx_src, dx_dst, send_sem.at[0], dx_sem, last)

    where_ld = pltpu.make_async_copy(where_ref, where_smem, in_sem.at[5])

    def tgt_copy():
        return remote(tgt_src, tgt_dst, send_sem.at[4], tgt_sem, 0)

    def label_logits():
        place = lax.broadcasted_iota(jnp.int32, (8, LANES), 1) * 8 + lax.broadcasted_iota(jnp.int32, (8, LANES), 0)
        where_ld.wait()

        def take(i, picked):
            out = []
            for c in range(chunks):
                top = where_smem[c, i] * 8
                out.append(jnp.where(place == where_smem[chunks + c, i], log_ref[pl.ds(top, 8), c * LANES:(c + 1) * LANES], picked[c]))
            return tuple(out)

        picked = lax.fori_loop(0, LANES, take, tuple(jnp.zeros((8, LANES), F) for _ in range(chunks)), unroll=8)
        for c in range(chunks):
            tgt_src[c:c + 1, :] = col_sum(picked[c])
        tgt_src[chunks:8, :] = jnp.zeros((8 - chunks, LANES), F)
        tgt_out[...] = tgt_src[...]
        tgt_copy().start()

    def part_copy(off):
        return remote(part_src, part_all.at[rank], many_sem, part_sem, 0, off)

    def greet():
        bar = pltpu.get_barrier_semaphore()
        for ds in range(stages):
            for off in range(tps):
                if ds or off:
                    pl.semaphore_signal(bar, inc=1, device_id={'pp': lax.rem(stage + ds, stages), 'tp': lax.rem(rank + off, tps)}, device_id_type=MESH)

    def met():
        pl.semaphore_wait(pltpu.get_barrier_semaphore(), stages * tps - 1)

    def normed(rows, gam, bet, start, size):
        hat, _ = ln_hat(rows)
        norm = (hat * gam + bet).astype(B)
        xh_out[start:start + size, :] = hat
        y_out[start:start + size, :] = norm
        yt_ref[:, start:start + size] = norm.astype(F).T.astype(B)

    def unpack(which):
        start = which * half
        normed(pack_dst[vecs + start:vecs + start + half, :], pack_dst[chunks:chunks + 1, :], pack_dst[chunks + 1:chunks + 2, :], start, half)
        if which == 0:
            lab_out[:chunks, :] = pack_dst[:chunks, :].astype(jnp.int32)

    def unpack_all():
        for w in range(2):
            pack_copy(helper, w, 0, pack_src).wait_recv()
            unpack(w)

    def st_sends(which):
        slot = 2 * rank + which
        return [remote(st_src, st_all.at[slot], many_sem, st_sem, lax.rem(stage + ds, stages), off) for ds in range(stages) for off in range(tps) if ds or off]

    def st_wait(count):
        got = st_all.at[pl.ds(0, count)]
        remote(got, got, many_sem, st_sem, last).wait_recv()

    def st_sent():
        sent = pack_src.at[pl.ds(0, 8 * (stages * tps - 1))]
        remote(sent, sent, many_sem, st_sem, last).wait_send()

    def finish_stats():
        tops = [st_all[r, 0:chunks, :] for r in range(2 * tps)]
        sums = [st_all[r, chunks:2 * chunks, :] for r in range(2 * tps)]
        top = functools.reduce(jnp.maximum, tops)
        tot = functools.reduce(jnp.add, [s * jnp.exp(t - top) for s, t in zip(sums, tops)])
        lse_out[:chunks, :] = top + jnp.log(tot)

    def logit_tile(row, size):
        logits = mm(e_ref[pl.ds(row, size), :], yt_ref[...])
        log_ref[pl.ds(row, size), :] = logits
        return logits

    def fill_logits(first, end):
        def step(i, carry):
            logit_tile(pl.multiple_of(i * TILE, TILE), TILE)
            return carry
        lax.fori_loop(first, end, step, 0, unroll=steps(end - first))

    def first_tiles(first, end):
        did = local_ids(did_out, chunks, rank * vocab, vocab)

        def fill(row, size):
            rows = tile_ids(row, size)
            one, zero = jnp.ones((size, LANES), B), jnp.zeros((size, LANES), B)
            h = [jnp.where(rows == did[:, c * LANES:(c + 1) * LANES], one, zero) for c in range(chunks)]
            first_ref[pl.ds(row, size), :] = mm(jnp.concatenate(h, axis=1), dx_out[...])

        def step(i, carry):
            fill(pl.multiple_of(i * TILE, TILE), TILE)
            return carry
        lax.fori_loop(first, end, step, 0, unroll=steps(end - first))
        if end == full:
            fill(full * TILE, tail)

    def logits_to(row, slot, top, size=TILE):
        logits = logit_tile(row, size)
        buf[slot, 0:size] = logits
        return jnp.maximum(top, jnp.max(logits.reshape(size // 8, 8, toks), axis=0))

    def add_exp(slot, top_old, top, tot, size=TILE):
        ex = jnp.exp(buf[slot, 0:size].reshape(size // 8, 8, toks) - top[None])
        return tot * jnp.exp(top_old - top) + jnp.sum(ex, axis=0)

    def begin_stats(first):
        low = jnp.full((8, toks), -jnp.inf, F)
        top = logits_to(first * TILE, 0, low)
        return top, top, jnp.zeros((8, toks), F)

    def run_stats(first, pairs, carry):
        def step(i, carry):
            old, top, tot = carry
            row = pl.multiple_of(first * TILE + i * 2 * TILE, TILE)
            mid = logits_to(row + TILE, 1, top)
            tot = add_exp(0, old, top, tot)
            new = logits_to(row + 2 * TILE, 0, mid)
            tot = add_exp(1, top, mid, tot)
            return mid, new, tot
        return lax.fori_loop(0, pairs, step, carry, unroll=steps(pairs))

    def share_stats(top, tot, which):
        high = jnp.max(top, axis=0, keepdims=True)
        tot = col_sum(tot * jnp.exp(top - high))
        for c in range(chunks):
            st_src[c:c + 1, :] = high[:, c * LANES:(c + 1) * LANES]
            st_src[chunks + c:chunks + c + 1, :] = tot[:, c * LANES:(c + 1) * LANES]
        st_all[2 * rank + which] = st_src[...]
        for send in st_sends(which):
            send.start()

    def mlp():
        ready(hid_ld, cot_ld, gam_ld, bet_ld, w1_ld, b1_ld, w2_ld)
        hat, _ = ln_hat(hid_ref[...].astype(F))
        norm = (hat * gam_ref[...] + bet_ref[...]).astype(B)
        pre = mm(norm, w1_ref[...]) + b1_ref[...]
        cube = 0.7978845608028654 * (pre + 0.044715 * (pre * pre * pre))
        th = jnp.tanh(cube)
        act = pre * (0.5 * (1.0 + th))
        slope = 0.5 * (1.0 + th) + pre * (0.5 * (1.0 - th * th)) * (0.7978845608028654 * (1.0 + 3 * 0.044715 * pre * pre))
        w2_out[...] = lax.dot_general(act.astype(B), cot_ref[...], TN, preferred_element_type=F)
        d_act = lax.dot_general(cot_ref[...], w2_ref[...], NT, preferred_element_type=F)
        d_pre = d_act * slope
        d_b = d_pre.astype(B)
        w1_out[...] = lax.dot_general(norm, d_b, TN, preferred_element_type=F)
        part_out[5:6, :] = col_sum(d_pre)
        d_h = lax.dot_general(d_b, w1_ref[...], NT, preferred_element_type=F)
        part_out[0:1, :] = col_sum(d_h * hat)
        part_out[1:2, :] = col_sum(d_h)
        part_out[2:5, :] = jnp.zeros((3, LANES), F)
        part_out[6:8, :] = jnp.zeros((2, LANES), F)

    @pl.when(stage == last)
    def _():
        fetch(hid_ld, ids_ld, gam_ld, bet_ld, e_parts[0])
        greet()
        ready(hid_ld, ids_ld, gam_ld, bet_ld)
        fetch(*e_parts[1:])
        rows = hid_ref[...].astype(F)
        pack_src[vecs:vecs + toks, :] = rows
        pack_src[:chunks, :] = ids_ref[...].astype(F)
        pack_src[chunks:chunks + 1, :] = gam_ref[...]
        pack_src[chunks + 1:chunks + 2, :] = bet_ref[...]
        pack_src[chunks + 2:vecs, :] = jnp.zeros((vecs - chunks - 2, dim), F)
        normed(rows, gam_ref[...], bet_ref[...], 0, toks)
        lab_out[:chunks, :] = ids_ref[...]
        e_parts[0].wait()
        row = jnp.clip(ids_ref[...] - rank * vocab, 0, vocab - 1)
        where_ref[:chunks, :] = row >> 3
        where_ref[chunks:2 * chunks, :] = lax.broadcasted_iota(jnp.int32, (chunks, LANES), 1) * 8 + (row & 7)
        where_ld.start()
        carry = run_stats(0, EARLY // 2, begin_stats(0))
        met()
        packs = pack_sends()
        for send in packs:
            send.start()
        ready(*e_parts[1:])
        old, top, tot = run_stats(EARLY, (SPLIT_STATS - 1 - EARLY) // 2, carry)
        tot = add_exp(0, old, top, tot)
        share_stats(top, tot, 0)
        fill_logits(SPLIT_STATS, full)
        logit_tile(full * TILE, tail)
        label_logits()
        dx_copy().wait_recv()
        dx_out[...] = dx_dst[:toks, :].astype(B)
        did_out[:chunks, :] = dx_dst[toks:toks + chunks, :].astype(jnp.int32)
        first_tiles(0, FIRST)
        st_wait(2 * tps - 1)
        finish_stats()
        for send in packs:
            send.wait_send()
        tgt_copy().wait_send()
        st_sent()

    @pl.when(stage == helper)
    def _():
        fetch(hid_ld, cot_ld, gam_ld, bet_ld, w1_ld, b1_ld, w2_ld, *e_parts)
        greet()
        mlp()
        met()
        ready(*e_parts)
        unpack_all()
        old, top, tot = run_stats(SPLIT_STATS, (full - 1 - SPLIT_STATS) // 2, begin_stats(SPLIT_STATS))
        new = logits_to(full * TILE, 1, top, tail)
        tot = add_exp(0, old, top, tot)
        tot = add_exp(1, top, new, tot, tail)
        share_stats(new, tot, 1)
        fill_logits(SPLIT_DY, SPLIT_STATS)
        st_wait(2 * tps - 1)
        finish_stats()
        st_sent()

    @pl.when(stage == 0)
    def _():
        fetch(cot_ld, ids_ld, gam_ld, smem_ld, *e_parts)
        greet()
        ready(cot_ld, ids_ld, gam_ld, smem_ld)

        def widen(i, carry):
            row = pl.multiple_of(i * TILE, TILE)
            e32_ref[pl.ds(row, TILE), :] = e_ref[pl.ds(row, TILE), :].astype(F)
            return carry

        for i in range(PARTS):
            e_parts[i].wait()
            lax.fori_loop(cuts[i], cuts[i + 1], widen, 0, unroll=4)
        e32_ref[full * TILE:vocab, :] = e_ref[full * TILE:vocab, :].astype(F)
        base = rank * vocab
        for c in range(chunks):
            def pick(i, carry):
                row = jnp.clip(ids_smem[c, i] - base, 0, vocab - 1)
                x_ref[pl.ds(c * LANES + i, 1), :] = e32_ref[pl.ds(row, 1), :]
                return carry
            lax.fori_loop(0, LANES, pick, 0, unroll=16)
        local = lanes_row(ids_ref, 0, chunks) - base
        inside = jnp.where((local >= 0) & (local < vocab), 1.0, 0.0)
        mask = jnp.broadcast_to(inside, (LANES, toks)).T
        hat, inv = ln_hat(x_ref[...])
        cot = cot_ref[...].astype(F)
        scaled = cot * gam_ref[...]
        grad = inv * (scaled - row_mean(scaled) - hat * row_mean(scaled * hat))
        grad = jnp.where(mask > 0.5, grad, 0.0).astype(B)
        dx_out[...] = grad
        did_out[:chunks, :] = ids_ref[...]
        dx_src[:toks, :] = grad.astype(F)
        dx_src[toks:toks + chunks, :] = ids_ref[...].astype(F)
        part_src[0:1, :] = col_sum(jnp.where(mask > 0.5, cot * hat, 0.0))
        part_src[1:2, :] = col_sum(jnp.where(mask > 0.5, cot, 0.0))
        part_src[2:8, :] = jnp.zeros((6, LANES), F)
        part_all[rank] = part_src[...]
        met()
        dx_copy().start()
        for off in range(1, tps):
            part_copy(off).start()
        first_tiles(0, full)
        sends = relays()
        for w in range(2):
            pack_copy(0, w, 0, pack_src).wait_recv()
            sends[w].start()
            unpack(w)
        fill_logits(0, full)
        logit_tile(full * TILE, tail)
        others = part_all.at[pl.ds(0, tps - 1)]
        remote(others, others, many_sem, part_sem, 0, 1).wait_recv()
        tgt_copy().wait_recv()
        tgt_out[...] = tgt_dst[...]
        part_out[...] = functools.reduce(jnp.add, [part_all[r] for r in range(tps)])
        st_wait(2 * tps)
        finish_stats()
        dx_copy().wait_send()
        for send in sends:
            send.wait_send()
        remote(others, others, many_sem, part_sem, 0, 1).wait_send()

    @pl.when((stage != 0) & (stage != helper) & (stage != last))
    def _():
        fetch(hid_ld, cot_ld, gam_ld, bet_ld, w1_ld, b1_ld, w2_ld, *e_parts)
        greet()
        mlp()
        met()
        ready(*e_parts)
        unpack_all()
        fill_logits(0, SPLIT_DY)
        st_wait(2 * tps)
        finish_stats()


def dy_piece(cfg, e_ref, log_ref, lab_ref, lse_ref, xh_ref, dyt_ref, part_ref, first, end, with_tail):
    stages, tps, toks, dim, vocab = cfg
    chunks = toks // LANES
    full, tail = vocab // TILE - 1, vocab - (vocab // TILE - 1) * TILE
    lse = lanes_row(lse_ref, 0, chunks)
    lab = lanes_row(lab_ref, 0, chunks) - lax.axis_index('tp') * vocab
    dyt_ref[...] = jnp.zeros((dim, toks), F)

    def work(row, size, seen):
        x = log_ref[pl.ds(row, size), :] - lse
        p = jnp.exp2(x * LOG2E)
        rows = lax.broadcasted_iota(jnp.int32, (size, LANES), 0) + row
        g, found = [], []
        for c in range(chunks):
            cols = slice(c * LANES, (c + 1) * LANES)
            hit = rows == lab[:, cols]
            pc, xc, at = p[:, cols], x[:, cols], seen[c]
            g.append(jnp.where(hit, pc - 1.0, pc).astype(B))
            for k in range(0, size, 8):
                at = jnp.where(hit[k:k + 8, :], xc[k:k + 8, :], at)
            found.append(at)
        dyt_ref[...] += lax.dot_general(e_ref[pl.ds(row, size), :], jnp.concatenate(g, axis=1), TN, preferred_element_type=F)
        return tuple(found)

    def step(i, seen):
        return work(pl.multiple_of(i * TILE, TILE), TILE, seen)

    seen = lax.fori_loop(first, end, step, tuple(jnp.zeros((8, LANES), F) for _ in range(chunks)), unroll=steps(end - first))
    if with_tail:
        seen = work(full * TILE, tail, seen)
    loss = functools.reduce(jnp.add, seen)
    dy = dyt_ref[...].T
    part_ref[2:3, :] += col_sum(dy * xh_ref[...])
    part_ref[3:4, :] += col_sum(dy)
    part_ref[4:5, :] += col_sum(loss)


def grad_kernel(cfg, e_ref, log_ref, first_ref, y_ref, lab_ref, lse_ref, dx_ref, did_ref, xh_ref, pin_ref, w1_in, w2_in, yt_ref, tgt_ref,
                emb_out, w1_out, b1_out, w2_out, part_out, out_ref, dyt_ref, zero_ref, bias_ref, o_sem, w_sem):
    stages, tps, toks, dim, vocab = cfg
    chunks = toks // LANES
    rank = lax.axis_index('tp')
    stage = lax.axis_index('pp')
    last = stages - 1
    helper = stages - 2
    base = rank * vocab
    full, tail = vocab // TILE - 1, vocab - (vocab // TILE - 1) * TILE
    bounds = (0, 16, 32, 44, full)
    spans = [(bounds[i], bounds[i + 1]) for i in range(4)]
    size16 = 16 * TILE

    def small(w1_src, w2_src):
        return [pltpu.make_async_copy(w1_src, w1_out, w_sem.at[0]), pltpu.make_async_copy(bias_ref, b1_out, w_sem.at[1]), pltpu.make_async_copy(w2_src, w2_out, w_sem.at[2])]

    @pl.when((stage == 0) | (stage == last))
    def _():
        zero_ref[...] = jnp.zeros(zero_ref.shape, F)
        bias_ref[...] = jnp.zeros(bias_ref.shape, F)
        smalls = small(zero_ref, zero_ref)
        for copy in smalls:
            copy.start()
        part_out[...] = pin_ref[...]
        lse = lanes_row(lse_ref, 0, chunks)
        lab = local_ids(lab_ref, chunks, base, vocab)
        did = local_ids(did_ref, chunks, base, vocab)
        less = jnp.exp2((lanes_row(tgt_ref, 0, chunks) - lse) * LOG2E) - 1.0
        less = [jnp.broadcast_to(less[:, c * LANES:(c + 1) * LANES], (16, LANES)).astype(B) for c in range(chunks)]

        def out_copy(c):
            start, size = (full * TILE, tail) if c == len(spans) else (spans[c][0] * TILE, (spans[c][1] - spans[c][0]) * TILE)
            return pltpu.make_async_copy(out_ref.at[pl.ds(start, size)], emb_out.at[pl.ds(start, size)], o_sem.at[c])

        def work(row, size, pick, fresh):
            logits = mm(e_ref[pl.ds(row, size), :], yt_ref[...]) if fresh else log_ref[pl.ds(row, size), :]
            p = jnp.exp2((logits - lse) * LOG2E)
            rows = tile_ids(row, size)
            one, zero = jnp.ones((size, LANES), B), jnp.zeros((size, LANES), B)
            g, h = [], []
            for c in range(chunks):
                cols = slice(c * LANES, (c + 1) * LANES)
                hit = jnp.concatenate([less[c]] * (size // 16), axis=0)
                g.append(jnp.where(rows == lab[:, cols], hit, p[:, cols].astype(B)))
                if pick:
                    h.append(jnp.where(rows == did[:, cols], one, zero))
            first = mm(jnp.concatenate(h, axis=1), dx_ref[...]) if pick else first_ref[pl.ds(row, size), :]
            out_ref[pl.ds(row, size), :] = first + mm(jnp.concatenate(g, axis=1), y_ref[...])

        def sweep(first, end, pick, fresh=False):
            def step(i, carry):
                work(pl.multiple_of(i * TILE, TILE), TILE, pick, fresh)
                return carry
            lax.fori_loop(first, end, step, 0, unroll=min(16, end - first))

        def both(run, fresh):
            pl.when(stage == 0)(lambda: run(False, fresh))
            pl.when(stage != 0)(lambda: run(True, False))

        both(lambda pick, fresh: work(full * TILE, tail, pick, fresh), False)
        out_copy(len(spans)).start()
        for c, (first, end) in enumerate(spans):
            if end <= FIRST:
                sweep(first, end, False)
            else:
                both(functools.partial(sweep, first, end), first >= FRESH)
            out_copy(c).start()
        for c in range(len(spans) + 1):
            out_copy(c).wait()
        for copy in smalls:
            copy.wait()

    @pl.when((stage != 0) & (stage != last))
    def _():
        out_ref[0:size16, :] = jnp.zeros((size16, dim), F)

        bias_ref[...] = pin_ref[5:6, :]
        zeros = [pltpu.make_async_copy(out_ref.at[pl.ds(0, n)], emb_out.at[pl.ds(c * size16, n)], o_sem.at[c]) for c, n in enumerate((size16, size16, size16, tail))]
        smalls = small(w1_in, w2_in)
        for copy in zeros + smalls:
            copy.start()
        part_out[...] = pin_ref[...]
        pieces = functools.partial(dy_piece, cfg, e_ref, log_ref, lab_ref, lse_ref, xh_ref, dyt_ref, part_out)

        @pl.when(stage == helper)
        def _():
            pieces(SPLIT_DY + LATE_HELPER, full, True)

        @pl.when(stage != helper)
        def _():
            pieces(LATE_FIRST, SPLIT_DY, False)

        for copy in zeros + smalls:
            copy.wait()


def sum_kernel(cfg, e_ref, log_ref, lab_ref, lse_ref, xh_ref, pin_ref, sum_out, part_ref, dyt_ref, got, send_sem, recv_sem):
    stages, tps, toks, dim, vocab = cfg
    rank = lax.axis_index('tp')
    stage = lax.axis_index('pp')
    last = stages - 1
    helper = stages - 2
    mids = helper
    bar = pltpu.get_barrier_semaphore()

    def copy_to(to_stage, off):
        slot = (stage - 1) * tps + rank
        return pltpu.make_async_remote_copy(part_ref, got.at[slot], send_sem, recv_sem, device_id={'pp': to_stage, 'tp': lax.rem(rank + off, tps)}, device_id_type=MESH)

    def batch(count):
        some = got.at[pl.ds(0, count)]
        return pltpu.make_async_remote_copy(some, some, send_sem, recv_sem, device_id={'tp': lax.rem(rank + 1, tps)}, device_id_type=MESH)

    def total(at):
        return functools.reduce(jnp.add, [got[at * tps + r] for r in range(tps)])

    @pl.when((stage != 0) & (stage != last))
    def _():
        for to_stage in range(1, 1 + mids):
            for off in range(tps):
                @pl.when((stage != to_stage) | (off != 0))
                def _():
                    pl.semaphore_signal(bar, inc=1, device_id={'pp': to_stage, 'tp': lax.rem(rank + off, tps)}, device_id_type=MESH)
        part_ref[...] = pin_ref[...]
        pieces = functools.partial(dy_piece, cfg, e_ref, log_ref, lab_ref, lse_ref, xh_ref, dyt_ref, part_ref)

        @pl.when(stage == helper)
        def _():
            pieces(SPLIT_DY, SPLIT_DY + LATE_HELPER, False)

        @pl.when(stage != helper)
        def _():
            pieces(0, LATE_FIRST, False)
        pl.semaphore_wait(bar, mids * tps - 1)

        @pl.when(stage == helper)
        def _():
            sends = [copy_to(helper, off) for off in range(1, tps)]
            for send in sends:
                send.start()
            got[(helper - 1) * tps + rank] = part_ref[...]
            batch(mids * tps - 1).wait_recv()
            own = total(helper - 1)
            rest = functools.reduce(jnp.add, [total(at) for at in range(helper)])
            sum_out[...] = jnp.concatenate([own[0:2, :], rest[2:8, :]], axis=0)
            batch(tps - 1).wait_send()

        @pl.when(stage != helper)
        def _():
            sends = [copy_to(helper, off) for off in range(tps)] + [copy_to(stage, off) for off in range(1, tps)]
            for send in sends:
                send.start()
            mine = (stage - 1) * tps
            got[mine + rank] = part_ref[...]
            batch(tps - 1).wait_recv()
            sum_out[...] = functools.reduce(jnp.add, [got[mine + r] for r in range(tps)])
            batch(2 * tps - 1).wait_send()

    @pl.when((stage == 0) | (stage == last))
    def _():
        sum_out[...] = pin_ref[...]


def hand_kernel(cfg, sum_ref, vec_out, got, send_sem, recv_sem):
    stages, tps, toks, dim, vocab = cfg
    stage = lax.axis_index('pp')
    last = stages - 1
    helper = stages - 2
    bar = pltpu.get_barrier_semaphore()

    def hand_over():
        return pltpu.make_async_remote_copy(sum_ref, got, send_sem, recv_sem, device_id={'pp': last}, device_id_type=MESH)

    @pl.when(stage == helper)
    def _():
        pl.semaphore_signal(bar, inc=1, device_id={'pp': last}, device_id_type=MESH)
        pl.semaphore_wait(bar, 1)
        hand_over().start()
        hand_over().wait_send()

    @pl.when(stage != last)
    def _():
        vec_out[0:2, :] = sum_ref[0:2, :]
        vec_out[2:3, :] = jnp.zeros((1, LANES), F)

    @pl.when(stage == last)
    def _():
        pl.semaphore_signal(bar, inc=1, device_id={'pp': helper}, device_id_type=MESH)
        pl.semaphore_wait(bar, 1)
        hand_over().wait_recv()
        vec_out[0:2, :] = got[2:4, :]
        vec_out[2:3, :] = got[4:5, :] * (-1.0 / toks)


def write_kernel(vec_ref, gam_out, bet_out, loss_out):
    gam_out[...] = vec_ref[0:1, :]
    bet_out[...] = vec_ref[1:2, :]
    loss_out[0] = jnp.sum(vec_ref[2:3, :])


def solution(mesh):
    stages, tps = mesh.shape['pp'], mesh.shape['tp']
    lead = ('dp', 'pp')
    hbm = pl.BlockSpec(memory_space=pltpu.HBM)
    vmem = pl.BlockSpec(memory_space=pltpu.VMEM)
    S = jax.ShapeDtypeStruct
    V = pltpu.VMEM
    DMA = pltpu.SemaphoreType.DMA
    I = jnp.int32

    def stay(*arrays):
        return [pltpu.with_memory_space_constraint(a, pltpu.HBM) for a in arrays]

    def body(tok_ids, hid_in, cot_in, ln_gamma, ln_beta, emb_table, w_in, b_in, w_out):
        dim = hid_in.shape[-1]
        hid = hid_in.reshape(-1, dim)
        cot = cot_in.reshape(-1, dim)
        toks = hid.shape[0]
        chunks = toks // LANES
        ids = tok_ids.reshape(chunks, LANES)
        table = emb_table[0]
        vocab = table.shape[0]
        ff = w_in.shape[2]
        cfg = (stages, tps, toks, dim, vocab)
        rows = toks + 2 * chunks
        vec = S((8, LANES), F)
        weights = (S((dim, ff), F), S((ff, dim), F))
        mids = pl.pallas_call(
            functools.partial(stats_kernel, cfg), name='stats',
            out_shape=(S((vocab, dim), B), S((vocab, toks), F), S((vocab, dim), F), S((toks, dim), B), S((8, LANES), I), vec, S((toks, dim), B), S((8, LANES), I), S((toks, dim), F), vec) + weights + (S((dim, toks), B), vec),
            in_specs=[hbm] * 9, out_specs=[vmem] * 14,
            scratch_shapes=[
                V((chunks, LANES), I), V((toks, dim), B), V((toks, dim), B), V((1, dim), F), V((1, dim), F), V((dim, ff), B), V((1, ff), F), V((ff, dim), B), pltpu.SMEM((chunks, LANES), I),
                V((2 * chunks, LANES), I), pltpu.SMEM((2 * chunks, LANES), I), V((8, LANES), F), V((8, LANES), F), V((2, TILE + 32, toks), F), V((rows, dim), F), V((rows, dim), F), V((rows, dim), F), V((rows, dim), F),
                V((8, LANES), F), V((2 * tps, 8, LANES), F), V((vocab, dim), F), V((toks, dim), F), V((8, LANES), F), V((tps, 8, LANES), F),
                DMA((PARTS,)), DMA((9,)), DMA((5,)), DMA, DMA((2,)), DMA, DMA, DMA, DMA],
            compiler_params=pltpu.CompilerParams(collective_id=0, has_side_effects=True, vmem_limit_bytes=GRANT),
        )(*stay(ids, hid, cot, ln_gamma, ln_beta, table, w_in[0], b_in, w_out[0]))
        emb_grad, w1g, b1g, w2g, part = pl.pallas_call(
            functools.partial(grad_kernel, cfg), name='grads',
            out_shape=(S((vocab, dim), F), S((dim, ff), F), S((1, ff), F), S((ff, dim), F), vec),
            in_specs=[vmem] * 14, out_specs=[hbm] * 4 + [vmem],
            scratch_shapes=[V((vocab, dim), F), V((dim, toks), F), V((dim, ff), F), V((1, ff), F), DMA((5,)), DMA((3,))],
            compiler_params=pltpu.CompilerParams(vmem_limit_bytes=GRANT),
        )(*mids)
        sums = pl.pallas_call(
            functools.partial(sum_kernel, cfg), name='sums', out_shape=vec, in_specs=[vmem] * 6, out_specs=vmem,
            scratch_shapes=[V((8, LANES), F), V((dim, toks), F), V(((stages - 2) * tps, 8, LANES), F), DMA, DMA],
            compiler_params=pltpu.CompilerParams(collective_id=1, has_side_effects=True, vmem_limit_bytes=GRANT),
        )(mids[0], mids[1], mids[4], mids[5], mids[8], part)
        vecs = pl.pallas_call(
            functools.partial(hand_kernel, cfg), name='hand', out_shape=vec, in_specs=[vmem], out_specs=vmem,
            scratch_shapes=[V((8, LANES), F), DMA, DMA],
            compiler_params=pltpu.CompilerParams(collective_id=2, has_side_effects=True, vmem_limit_bytes=4 << 20),
        )(sums)
        gam, bet, loss = pl.pallas_call(
            write_kernel, name='write', out_shape=(S((1, dim), F), S((1, dim), F), S((1,), F)), in_specs=[vmem], out_specs=[vmem] * 2 + [pl.BlockSpec(memory_space=pltpu.SMEM)],
            compiler_params=pltpu.CompilerParams(vmem_limit_bytes=4 << 20),
        )(vecs)
        return emb_grad[None], loss, gam, bet, w1g[None], b1g, w2g[None]

    rows, cols = P(lead, 'tp'), P(lead, None, 'tp')
    specs_in = (P(lead),) * 5 + (rows, cols, rows, rows)
    specs_out = (rows, P(lead), P(lead), P(lead), cols, rows, rows)
    return jax.shard_map(body, mesh=mesh, in_specs=specs_in, out_specs=specs_out, check_vma=False)
```

```python
import functools

import jax
import jax.numpy as jnp
from jax import lax
from jax.experimental import pallas as pl
from jax.experimental.pallas import tpu as pltpu
from jax.sharding import PartitionSpec as P

F = jnp.float32
B = jnp.bfloat16
LN_EPS = 1e-5
LOG2E = 1.4426950408889634
LANES = 128
TILE = 256
SPLIT_STATS = 37
SPLIT_DY = 20
EARLY = 8
FIRST = 16
FRESH = 48
PARTS = 4
LATE_HELPER = 12
LATE_FIRST = 8
GRANT = 14 << 20
MESH = pl.DeviceIdType.MESH
NT = (((1,), (1,)), ((), ()))
TN = (((0,), (0,)), ((), ()))


def col_sum(values):
    return jnp.sum(values, axis=0, keepdims=True)


def row_mean(values):
    return jnp.mean(values, axis=-1, keepdims=True)


def ln_hat(rows):
    centre = rows - row_mean(rows)
    inv = lax.rsqrt(row_mean(centre * centre) + LN_EPS)
    return centre * inv, inv


def tile_ids(row, size):
    return (lax.broadcasted_iota(jnp.int32, (size, LANES), 0) + row).astype(jnp.int16)


def local_ids(ref, chunks, base, vocab):
    ids = lanes_row(ref, 0, chunks) - base
    return jnp.where((ids >= 0) & (ids < vocab), ids, -1).astype(jnp.int16)


def steps(count):
    return max(d for d in range(1, 14) if count % d == 0)


def mm(a, b):
    return jnp.dot(a, b, preferred_element_type=F)


def lanes_row(ref, first, chunks):
    return jnp.concatenate([ref[first + c:first + c + 1, :] for c in range(chunks)], axis=1)


def stats_kernel(cfg, ids_hbm, hid_hbm, cot_hbm, gam_hbm, bet_hbm, emb_hbm, w1_hbm, b1_hbm, w2_hbm,
                 e_ref, log_ref, first_ref, y_out, lab_out, lse_out, dx_out, did_out, xh_out, part_out, w1_out, w2_out, yt_ref, tgt_out,
                 ids_ref, hid_ref, cot_ref, gam_ref, bet_ref, w1_ref, b1_ref, w2_ref, ids_smem,
                 where_ref, where_smem, tgt_src, tgt_dst, buf, pack_src, pack_dst, dx_src, dx_dst, st_src, st_all, e32_ref, x_ref, part_src, part_all,
                 e_sem, in_sem, send_sem, many_sem, pack_sem, dx_sem, st_sem, part_sem, tgt_sem):
    stages, tps, toks, dim, vocab = cfg
    chunks = toks // LANES
    rank = lax.axis_index('tp')
    stage = lax.axis_index('pp')
    last = stages - 1
    helper = stages - 2
    full, tail = vocab // TILE - 1, vocab - (vocab // TILE - 1) * TILE
    vecs = 2 * chunks
    half = toks // 2
    cuts = [i * (full // PARTS) for i in range(PARTS)] + [full]

    def e_part(i):
        start = cuts[i] * TILE
        size = (vocab if i == PARTS - 1 else cuts[i + 1] * TILE) - start
        return pltpu.make_async_copy(emb_hbm.at[pl.ds(start, size)], e_ref.at[pl.ds(start, size)], e_sem.at[i])

    e_parts = [e_part(i) for i in range(PARTS)]
    pairs = ((hid_hbm, hid_ref), (ids_hbm, ids_ref), (gam_hbm, gam_ref), (bet_hbm, bet_ref), (cot_hbm, cot_ref), (ids_hbm, ids_smem), (w1_hbm, w1_ref), (b1_hbm, b1_ref), (w2_hbm, w2_ref))
    hid_ld, ids_ld, gam_ld, bet_ld, cot_ld, smem_ld, w1_ld, b1_ld, w2_ld = [pltpu.make_async_copy(a, b, in_sem.at[i]) for i, (a, b) in enumerate(pairs)]

    def fetch(*copies):
        for copy in copies:
            copy.start()

    def ready(*copies):
        for copy in copies:
            copy.wait()

    def remote(src, dst, ssem, rsem, to_stage, off=0):
        return pltpu.make_async_remote_copy(src, dst, ssem, rsem, device_id={'pp': to_stage, 'tp': lax.rem(rank + off, tps)}, device_id_type=MESH)

    def pack_rows(which):
        return pl.ds(0, vecs + half) if which == 0 else pl.ds(vecs + half, half)

    def pack_copy(to_stage, which, idx, src):
        return remote(src.at[pack_rows(which)], pack_dst.at[pack_rows(which)], send_sem.at[idx], pack_sem.at[which], to_stage)

    def pack_sends():
        return [pack_copy(helper, 0, 0, pack_src), pack_copy(helper, 1, 1, pack_src), pack_copy(0, 0, 2, pack_src), pack_copy(0, 1, 3, pack_src)]

    def relays():
        return [pack_copy(1, w, 1 + w, pack_dst) for w in range(2)]

    def dx_copy():
        return remote(dx_src, dx_dst, send_sem.at[0], dx_sem, last)

    where_ld = pltpu.make_async_copy(where_ref, where_smem, in_sem.at[5])

    def tgt_copy():
        return remote(tgt_src, tgt_dst, send_sem.at[4], tgt_sem, 0)

    def label_logits():
        place = lax.broadcasted_iota(jnp.int32, (8, LANES), 1) * 8 + lax.broadcasted_iota(jnp.int32, (8, LANES), 0)
        where_ld.wait()

        def take(i, picked):
            out = []
            for c in range(chunks):
                top = where_smem[c, i] * 8
                out.append(jnp.where(place == where_smem[chunks + c, i], log_ref[pl.ds(top, 8), c * LANES:(c + 1) * LANES], picked[c]))
            return tuple(out)

        picked = lax.fori_loop(0, LANES, take, tuple(jnp.zeros((8, LANES), F) for _ in range(chunks)), unroll=8)
        for c in range(chunks):
            tgt_src[c:c + 1, :] = col_sum(picked[c])
        tgt_src[chunks:8, :] = jnp.zeros((8 - chunks, LANES), F)
        tgt_out[...] = tgt_src[...]
        tgt_copy().start()

    def part_copy(off):
        return remote(part_src, part_all.at[rank], many_sem, part_sem, 0, off)

    def greet():
        bar = pltpu.get_barrier_semaphore()
        for ds in range(stages):
            for off in range(tps):
                if ds or off:
                    pl.semaphore_signal(bar, inc=1, device_id={'pp': lax.rem(stage + ds, stages), 'tp': lax.rem(rank + off, tps)}, device_id_type=MESH)

    def met():
        pl.semaphore_wait(pltpu.get_barrier_semaphore(), stages * tps - 1)

    def normed(rows, gam, bet, start, size):
        hat, _ = ln_hat(rows)
        norm = (hat * gam + bet).astype(B)
        xh_out[start:start + size, :] = hat
        y_out[start:start + size, :] = norm
        yt_ref[:, start:start + size] = norm.astype(F).T.astype(B)

    def unpack(which):
        start = which * half
        normed(pack_dst[vecs + start:vecs + start + half, :], pack_dst[chunks:chunks + 1, :], pack_dst[chunks + 1:chunks + 2, :], start, half)
        if which == 0:
            lab_out[:chunks, :] = pack_dst[:chunks, :].astype(jnp.int32)

    def unpack_all():
        for w in range(2):
            pack_copy(helper, w, 0, pack_src).wait_recv()
            unpack(w)

    def st_sends(which):
        slot = 2 * rank + which
        return [remote(st_src, st_all.at[slot], many_sem, st_sem, lax.rem(stage + ds, stages), off) for ds in range(stages) for off in range(tps) if ds or off]

    def st_wait(count):
        got = st_all.at[pl.ds(0, count)]
        remote(got, got, many_sem, st_sem, last).wait_recv()

    def st_sent():
        sent = pack_src.at[pl.ds(0, 8 * (stages * tps - 1))]
        remote(sent, sent, many_sem, st_sem, last).wait_send()

    def finish_stats():
        tops = [st_all[r, 0:chunks, :] for r in range(2 * tps)]
        sums = [st_all[r, chunks:2 * chunks, :] for r in range(2 * tps)]
        top = functools.reduce(jnp.maximum, tops)
        tot = functools.reduce(jnp.add, [s * jnp.exp(t - top) for s, t in zip(sums, tops)])
        lse_out[:chunks, :] = top + jnp.log(tot)

    def logit_tile(row, size):
        logits = mm(e_ref[pl.ds(row, size), :], yt_ref[...])
        log_ref[pl.ds(row, size), :] = logits
        return logits

    def fill_logits(first, end):
        def step(i, carry):
            logit_tile(pl.multiple_of(i * TILE, TILE), TILE)
            return carry
        lax.fori_loop(first, end, step, 0, unroll=steps(end - first))

    def first_tiles(first, end):
        did = local_ids(did_out, chunks, rank * vocab, vocab)

        def fill(row, size):
            rows = tile_ids(row, size)
            one, zero = jnp.ones((size, LANES), B), jnp.zeros((size, LANES), B)
            h = [jnp.where(rows == did[:, c * LANES:(c + 1) * LANES], one, zero) for c in range(chunks)]
            first_ref[pl.ds(row, size), :] = mm(jnp.concatenate(h, axis=1), dx_out[...])

        def step(i, carry):
            fill(pl.multiple_of(i * TILE, TILE), TILE)
            return carry
        lax.fori_loop(first, end, step, 0, unroll=steps(end - first))
        if end == full:
            fill(full * TILE, tail)

    def logits_to(row, slot, top, size=TILE):
        logits = logit_tile(row, size)
        buf[slot, 0:size] = logits
        return jnp.maximum(top, jnp.max(logits.reshape(size // 8, 8, toks), axis=0))

    def add_exp(slot, top_old, top, tot, size=TILE):
        ex = jnp.exp(buf[slot, 0:size].reshape(size // 8, 8, toks) - top[None])
        return tot * jnp.exp(top_old - top) + jnp.sum(ex, axis=0)

    def begin_stats(first):
        low = jnp.full((8, toks), -jnp.inf, F)
        top = logits_to(first * TILE, 0, low)
        return top, top, jnp.zeros((8, toks), F)

    def run_stats(first, pairs, carry):
        def step(i, carry):
            old, top, tot = carry
            row = pl.multiple_of(first * TILE + i * 2 * TILE, TILE)
            mid = logits_to(row + TILE, 1, top)
            tot = add_exp(0, old, top, tot)
            new = logits_to(row + 2 * TILE, 0, mid)
            tot = add_exp(1, top, mid, tot)
            return mid, new, tot
        return lax.fori_loop(0, pairs, step, carry, unroll=steps(pairs))

    def share_stats(top, tot, which):
        high = jnp.max(top, axis=0, keepdims=True)
        tot = col_sum(tot * jnp.exp(top - high))
        for c in range(chunks):
            st_src[c:c + 1, :] = high[:, c * LANES:(c + 1) * LANES]
            st_src[chunks + c:chunks + c + 1, :] = tot[:, c * LANES:(c + 1) * LANES]
        st_all[2 * rank + which] = st_src[...]
        for send in st_sends(which):
            send.start()

    def mlp():
        ready(hid_ld, cot_ld, gam_ld, bet_ld, w1_ld, b1_ld, w2_ld)
        hat, _ = ln_hat(hid_ref[...].astype(F))
        norm = (hat * gam_ref[...] + bet_ref[...]).astype(B)
        pre = mm(norm, w1_ref[...]) + b1_ref[...]
        cube = 0.7978845608028654 * (pre + 0.044715 * (pre * pre * pre))
        th = jnp.tanh(cube)
        act = pre * (0.5 * (1.0 + th))
        slope = 0.5 * (1.0 + th) + pre * (0.5 * (1.0 - th * th)) * (0.7978845608028654 * (1.0 + 3 * 0.044715 * pre * pre))
        w2_out[...] = lax.dot_general(act.astype(B), cot_ref[...], TN, preferred_element_type=F)
        d_act = lax.dot_general(cot_ref[...], w2_ref[...], NT, preferred_element_type=F)
        d_pre = d_act * slope
        d_b = d_pre.astype(B)
        w1_out[...] = lax.dot_general(norm, d_b, TN, preferred_element_type=F)
        part_out[5:6, :] = col_sum(d_pre)
        d_h = lax.dot_general(d_b, w1_ref[...], NT, preferred_element_type=F)
        part_out[0:1, :] = col_sum(d_h * hat)
        part_out[1:2, :] = col_sum(d_h)
        part_out[2:5, :] = jnp.zeros((3, LANES), F)
        part_out[6:8, :] = jnp.zeros((2, LANES), F)

    @pl.when(stage == last)
    def _():
        fetch(hid_ld, ids_ld, gam_ld, bet_ld, e_parts[0])
        greet()
        ready(hid_ld, ids_ld, gam_ld, bet_ld)
        fetch(*e_parts[1:])
        rows = hid_ref[...].astype(F)
        pack_src[vecs:vecs + toks, :] = rows
        pack_src[:chunks, :] = ids_ref[...].astype(F)
        pack_src[chunks:chunks + 1, :] = gam_ref[...]
        pack_src[chunks + 1:chunks + 2, :] = bet_ref[...]
        pack_src[chunks + 2:vecs, :] = jnp.zeros((vecs - chunks - 2, dim), F)
        normed(rows, gam_ref[...], bet_ref[...], 0, toks)
        lab_out[:chunks, :] = ids_ref[...]
        e_parts[0].wait()
        row = jnp.clip(ids_ref[...] - rank * vocab, 0, vocab - 1)
        where_ref[:chunks, :] = row >> 3
        where_ref[chunks:2 * chunks, :] = lax.broadcasted_iota(jnp.int32, (chunks, LANES), 1) * 8 + (row & 7)
        where_ld.start()
        carry = run_stats(0, EARLY // 2, begin_stats(0))
        met()
        packs = pack_sends()
        for send in packs:
            send.start()
        ready(*e_parts[1:])
        old, top, tot = run_stats(EARLY, (SPLIT_STATS - 1 - EARLY) // 2, carry)
        tot = add_exp(0, old, top, tot)
        share_stats(top, tot, 0)
        fill_logits(SPLIT_STATS, full)
        logit_tile(full * TILE, tail)
        label_logits()
        dx_copy().wait_recv()
        dx_out[...] = dx_dst[:toks, :].astype(B)
        did_out[:chunks, :] = dx_dst[toks:toks + chunks, :].astype(jnp.int32)
        first_tiles(0, FIRST)
        st_wait(2 * tps - 1)
        finish_stats()
        for send in packs:
            send.wait_send()
        tgt_copy().wait_send()
        st_sent()

    @pl.when(stage == helper)
    def _():
        fetch(hid_ld, cot_ld, gam_ld, bet_ld, w1_ld, b1_ld, w2_ld, *e_parts)
        greet()
        mlp()
        met()
        ready(*e_parts)
        unpack_all()
        old, top, tot = run_stats(SPLIT_STATS, (full - 1 - SPLIT_STATS) // 2, begin_stats(SPLIT_STATS))
        new = logits_to(full * TILE, 1, top, tail)
        tot = add_exp(0, old, top, tot)
        tot = add_exp(1, top, new, tot, tail)
        share_stats(new, tot, 1)
        fill_logits(SPLIT_DY, SPLIT_STATS)
        st_wait(2 * tps - 1)
        finish_stats()
        st_sent()

    @pl.when(stage == 0)
    def _():
        fetch(cot_ld, ids_ld, gam_ld, smem_ld, *e_parts)
        greet()
        ready(cot_ld, ids_ld, gam_ld, smem_ld)

        def widen(i, carry):
            row = pl.multiple_of(i * TILE, TILE)
            e32_ref[pl.ds(row, TILE), :] = e_ref[pl.ds(row, TILE), :].astype(F)
            return carry

        for i in range(PARTS):
            e_parts[i].wait()
            lax.fori_loop(cuts[i], cuts[i + 1], widen, 0, unroll=4)
        e32_ref[full * TILE:vocab, :] = e_ref[full * TILE:vocab, :].astype(F)
        base = rank * vocab
        for c in range(chunks):
            def pick(i, carry):
                row = jnp.clip(ids_smem[c, i] - base, 0, vocab - 1)
                x_ref[pl.ds(c * LANES + i, 1), :] = e32_ref[pl.ds(row, 1), :]
                return carry
            lax.fori_loop(0, LANES, pick, 0, unroll=16)
        local = lanes_row(ids_ref, 0, chunks) - base
        inside = jnp.where((local >= 0) & (local < vocab), 1.0, 0.0)
        mask = jnp.broadcast_to(inside, (LANES, toks)).T
        hat, inv = ln_hat(x_ref[...])
        cot = cot_ref[...].astype(F)
        scaled = cot * gam_ref[...]
        grad = inv * (scaled - row_mean(scaled) - hat * row_mean(scaled * hat))
        grad = jnp.where(mask > 0.5, grad, 0.0).astype(B)
        dx_out[...] = grad
        did_out[:chunks, :] = ids_ref[...]
        dx_src[:toks, :] = grad.astype(F)
        dx_src[toks:toks + chunks, :] = ids_ref[...].astype(F)
        part_src[0:1, :] = col_sum(jnp.where(mask > 0.5, cot * hat, 0.0))
        part_src[1:2, :] = col_sum(jnp.where(mask > 0.5, cot, 0.0))
        part_src[2:8, :] = jnp.zeros((6, LANES), F)
        part_all[rank] = part_src[...]
        met()
        dx_copy().start()
        for off in range(1, tps):
            part_copy(off).start()
        first_tiles(0, full)
        sends = relays()
        for w in range(2):
            pack_copy(0, w, 0, pack_src).wait_recv()
            sends[w].start()
            unpack(w)
        fill_logits(0, full)
        logit_tile(full * TILE, tail)
        others = part_all.at[pl.ds(0, tps - 1)]
        remote(others, others, many_sem, part_sem, 0, 1).wait_recv()
        tgt_copy().wait_recv()
        tgt_out[...] = tgt_dst[...]
        part_out[...] = functools.reduce(jnp.add, [part_all[r] for r in range(tps)])
        st_wait(2 * tps)
        finish_stats()
        dx_copy().wait_send()
        for send in sends:
            send.wait_send()
        remote(others, others, many_sem, part_sem, 0, 1).wait_send()

    @pl.when((stage != 0) & (stage != helper) & (stage != last))
    def _():
        fetch(hid_ld, cot_ld, gam_ld, bet_ld, w1_ld, b1_ld, w2_ld, *e_parts)
        greet()
        mlp()
        met()
        ready(*e_parts)
        unpack_all()
        fill_logits(0, SPLIT_DY)
        st_wait(2 * tps)
        finish_stats()


def dy_piece(cfg, e_ref, log_ref, lab_ref, lse_ref, xh_ref, dyt_ref, part_ref, first, end, with_tail):
    stages, tps, toks, dim, vocab = cfg
    chunks = toks // LANES
    full, tail = vocab // TILE - 1, vocab - (vocab // TILE - 1) * TILE
    lse = lanes_row(lse_ref, 0, chunks)
    lab = lanes_row(lab_ref, 0, chunks) - lax.axis_index('tp') * vocab
    dyt_ref[...] = jnp.zeros((dim, toks), F)

    def work(row, size, seen):
        x = log_ref[pl.ds(row, size), :] - lse
        p = jnp.exp2(x * LOG2E)
        rows = lax.broadcasted_iota(jnp.int32, (size, LANES), 0) + row
        g, found = [], []
        for c in range(chunks):
            cols = slice(c * LANES, (c + 1) * LANES)
            hit = rows == lab[:, cols]
            pc, xc, at = p[:, cols], x[:, cols], seen[c]
            g.append(jnp.where(hit, pc - 1.0, pc).astype(B))
            for k in range(0, size, 8):
                at = jnp.where(hit[k:k + 8, :], xc[k:k + 8, :], at)
            found.append(at)
        dyt_ref[...] += lax.dot_general(e_ref[pl.ds(row, size), :], jnp.concatenate(g, axis=1), TN, preferred_element_type=F)
        return tuple(found)

    def step(i, seen):
        return work(pl.multiple_of(i * TILE, TILE), TILE, seen)

    seen = lax.fori_loop(first, end, step, tuple(jnp.zeros((8, LANES), F) for _ in range(chunks)), unroll=steps(end - first))
    if with_tail:
        seen = work(full * TILE, tail, seen)
    loss = functools.reduce(jnp.add, seen)
    dy = dyt_ref[...].T
    part_ref[2:3, :] += col_sum(dy * xh_ref[...])
    part_ref[3:4, :] += col_sum(dy)
    part_ref[4:5, :] += col_sum(loss)


def grad_kernel(cfg, e_ref, log_ref, first_ref, y_ref, lab_ref, lse_ref, dx_ref, did_ref, xh_ref, pin_ref, w1_in, w2_in, yt_ref, tgt_ref,
                emb_out, w1_out, b1_out, w2_out, part_out, out_ref, dyt_ref, zero_ref, bias_ref, o_sem, w_sem):
    stages, tps, toks, dim, vocab = cfg
    chunks = toks // LANES
    rank = lax.axis_index('tp')
    stage = lax.axis_index('pp')
    last = stages - 1
    helper = stages - 2
    base = rank * vocab
    full, tail = vocab // TILE - 1, vocab - (vocab // TILE - 1) * TILE
    bounds = (0, 16, 32, 44, full)
    spans = [(bounds[i], bounds[i + 1]) for i in range(4)]
    size16 = 16 * TILE

    def small(w1_src, w2_src):
        return [pltpu.make_async_copy(w1_src, w1_out, w_sem.at[0]), pltpu.make_async_copy(bias_ref, b1_out, w_sem.at[1]), pltpu.make_async_copy(w2_src, w2_out, w_sem.at[2])]

    @pl.when((stage == 0) | (stage == last))
    def _():
        zero_ref[...] = jnp.zeros(zero_ref.shape, F)
        bias_ref[...] = jnp.zeros(bias_ref.shape, F)
        smalls = small(zero_ref, zero_ref)
        for copy in smalls:
            copy.start()
        part_out[...] = pin_ref[...]
        lse = lanes_row(lse_ref, 0, chunks)
        lab = local_ids(lab_ref, chunks, base, vocab)
        did = local_ids(did_ref, chunks, base, vocab)
        less = jnp.exp2((lanes_row(tgt_ref, 0, chunks) - lse) * LOG2E) - 1.0
        less = [jnp.broadcast_to(less[:, c * LANES:(c + 1) * LANES], (16, LANES)).astype(B) for c in range(chunks)]

        def out_copy(c):
            start, size = (full * TILE, tail) if c == len(spans) else (spans[c][0] * TILE, (spans[c][1] - spans[c][0]) * TILE)
            return pltpu.make_async_copy(out_ref.at[pl.ds(start, size)], emb_out.at[pl.ds(start, size)], o_sem.at[c])

        def work(row, size, pick, fresh):
            logits = mm(e_ref[pl.ds(row, size), :], yt_ref[...]) if fresh else log_ref[pl.ds(row, size), :]
            p = jnp.exp2((logits - lse) * LOG2E)
            rows = tile_ids(row, size)
            one, zero = jnp.ones((size, LANES), B), jnp.zeros((size, LANES), B)
            g, h = [], []
            for c in range(chunks):
                cols = slice(c * LANES, (c + 1) * LANES)
                hit = jnp.concatenate([less[c]] * (size // 16), axis=0)
                g.append(jnp.where(rows == lab[:, cols], hit, p[:, cols].astype(B)))
                if pick:
                    h.append(jnp.where(rows == did[:, cols], one, zero))
            first = mm(jnp.concatenate(h, axis=1), dx_ref[...]) if pick else first_ref[pl.ds(row, size), :]
            out_ref[pl.ds(row, size), :] = first + mm(jnp.concatenate(g, axis=1), y_ref[...])

        def sweep(first, end, pick, fresh=False):
            def step(i, carry):
                work(pl.multiple_of(i * TILE, TILE), TILE, pick, fresh)
                return carry
            lax.fori_loop(first, end, step, 0, unroll=min(16, end - first))

        def both(run, fresh):
            pl.when(stage == 0)(lambda: run(False, fresh))
            pl.when(stage != 0)(lambda: run(True, False))

        both(lambda pick, fresh: work(full * TILE, tail, pick, fresh), False)
        out_copy(len(spans)).start()
        for c, (first, end) in enumerate(spans):
            if end <= FIRST:
                sweep(first, end, False)
            else:
                both(functools.partial(sweep, first, end), first >= FRESH)
            out_copy(c).start()
        for c in range(len(spans) + 1):
            out_copy(c).wait()
        for copy in smalls:
            copy.wait()

    @pl.when((stage != 0) & (stage != last))
    def _():
        out_ref[0:size16, :] = jnp.zeros((size16, dim), F)

        bias_ref[...] = pin_ref[5:6, :]
        zeros = [pltpu.make_async_copy(out_ref.at[pl.ds(0, n)], emb_out.at[pl.ds(c * size16, n)], o_sem.at[c]) for c, n in enumerate((size16, size16, size16, tail))]
        smalls = small(w1_in, w2_in)
        for copy in zeros + smalls:
            copy.start()
        part_out[...] = pin_ref[...]
        pieces = functools.partial(dy_piece, cfg, e_ref, log_ref, lab_ref, lse_ref, xh_ref, dyt_ref, part_out)

        @pl.when(stage == helper)
        def _():
            pieces(SPLIT_DY + LATE_HELPER, full, True)

        @pl.when(stage != helper)
        def _():
            pieces(LATE_FIRST, SPLIT_DY, False)

        for copy in zeros + smalls:
            copy.wait()


def sum_kernel(cfg, e_ref, log_ref, lab_ref, lse_ref, xh_ref, pin_ref, sum_out, part_ref, dyt_ref, got, send_sem, recv_sem):
    stages, tps, toks, dim, vocab = cfg
    rank = lax.axis_index('tp')
    stage = lax.axis_index('pp')
    last = stages - 1
    helper = stages - 2
    mids = helper
    bar = pltpu.get_barrier_semaphore()

    def copy_to(to_stage, off):
        slot = (stage - 1) * tps + rank
        return pltpu.make_async_remote_copy(part_ref, got.at[slot], send_sem, recv_sem, device_id={'pp': to_stage, 'tp': lax.rem(rank + off, tps)}, device_id_type=MESH)

    def batch(count):
        some = got.at[pl.ds(0, count)]
        return pltpu.make_async_remote_copy(some, some, send_sem, recv_sem, device_id={'tp': lax.rem(rank + 1, tps)}, device_id_type=MESH)

    def total(at):
        return functools.reduce(jnp.add, [got[at * tps + r] for r in range(tps)])

    @pl.when((stage != 0) & (stage != last))
    def _():
        for to_stage in range(1, 1 + mids):
            for off in range(tps):
                @pl.when((stage != to_stage) | (off != 0))
                def _():
                    pl.semaphore_signal(bar, inc=1, device_id={'pp': to_stage, 'tp': lax.rem(rank + off, tps)}, device_id_type=MESH)
        part_ref[...] = pin_ref[...]
        pieces = functools.partial(dy_piece, cfg, e_ref, log_ref, lab_ref, lse_ref, xh_ref, dyt_ref, part_ref)

        @pl.when(stage == helper)
        def _():
            pieces(SPLIT_DY, SPLIT_DY + LATE_HELPER, False)

        @pl.when(stage != helper)
        def _():
            pieces(0, LATE_FIRST, False)
        pl.semaphore_wait(bar, mids * tps - 1)

        @pl.when(stage == helper)
        def _():
            sends = [copy_to(helper, off) for off in range(1, tps)]
            for send in sends:
                send.start()
            got[(helper - 1) * tps + rank] = part_ref[...]
            batch(mids * tps - 1).wait_recv()
            own = total(helper - 1)
            rest = functools.reduce(jnp.add, [total(at) for at in range(helper)])
            sum_out[...] = jnp.concatenate([own[0:2, :], rest[2:8, :]], axis=0)
            batch(tps - 1).wait_send()

        @pl.when(stage != helper)
        def _():
            sends = [copy_to(helper, off) for off in range(tps)] + [copy_to(stage, off) for off in range(1, tps)]
            for send in sends:
                send.start()
            mine = (stage - 1) * tps
            got[mine + rank] = part_ref[...]
            batch(tps - 1).wait_recv()
            sum_out[...] = functools.reduce(jnp.add, [got[mine + r] for r in range(tps)])
            batch(2 * tps - 1).wait_send()

    @pl.when((stage == 0) | (stage == last))
    def _():
        sum_out[...] = pin_ref[...]


def hand_kernel(cfg, sum_ref, vec_out, got, send_sem, recv_sem):
    stages, tps, toks, dim, vocab = cfg
    stage = lax.axis_index('pp')
    last = stages - 1
    helper = stages - 2
    bar = pltpu.get_barrier_semaphore()

    def hand_over():
        return pltpu.make_async_remote_copy(sum_ref, got, send_sem, recv_sem, device_id={'pp': last}, device_id_type=MESH)

    @pl.when(stage == helper)
    def _():
        pl.semaphore_signal(bar, inc=1, device_id={'pp': last}, device_id_type=MESH)
        pl.semaphore_wait(bar, 1)
        hand_over().start()
        hand_over().wait_send()

    @pl.when(stage != last)
    def _():
        vec_out[0:2, :] = sum_ref[0:2, :]
        vec_out[2:3, :] = jnp.zeros((1, LANES), F)

    @pl.when(stage == last)
    def _():
        pl.semaphore_signal(bar, inc=1, device_id={'pp': helper}, device_id_type=MESH)
        pl.semaphore_wait(bar, 1)
        hand_over().wait_recv()
        vec_out[0:2, :] = got[2:4, :]
        vec_out[2:3, :] = got[4:5, :] * (-1.0 / toks)


def write_kernel(vec_ref, gam_out, bet_out, loss_out):
    gam_out[...] = vec_ref[0:1, :]
    bet_out[...] = vec_ref[1:2, :]
    loss_out[0] = jnp.sum(vec_ref[2:3, :])


def solution(mesh):
    stages, tps = mesh.shape['pp'], mesh.shape['tp']
    lead = ('dp', 'pp')
    hbm = pl.BlockSpec(memory_space=pltpu.HBM)
    vmem = pl.BlockSpec(memory_space=pltpu.VMEM)
    S = jax.ShapeDtypeStruct
    V = pltpu.VMEM
    DMA = pltpu.SemaphoreType.DMA
    I = jnp.int32

    def stay(*arrays):
        return [pltpu.with_memory_space_constraint(a, pltpu.HBM) for a in arrays]

    def body(tok_ids, hid_in, cot_in, ln_gamma, ln_beta, emb_table, w_in, b_in, w_out):
        dim = hid_in.shape[-1]
        hid = hid_in.reshape(-1, dim)
        cot = cot_in.reshape(-1, dim)
        toks = hid.shape[0]
        chunks = toks // LANES
        ids = tok_ids.reshape(chunks, LANES)
        table = emb_table[0]
        vocab = table.shape[0]
        ff = w_in.shape[2]
        cfg = (stages, tps, toks, dim, vocab)
        rows = toks + 2 * chunks
        vec = S((8, LANES), F)
        weights = (S((dim, ff), F), S((ff, dim), F))
        mids = pl.pallas_call(
            functools.partial(stats_kernel, cfg), name='stats',
            out_shape=(S((vocab, dim), B), S((vocab, toks), F), S((vocab, dim), F), S((toks, dim), B), S((8, LANES), I), vec, S((toks, dim), B), S((8, LANES), I), S((toks, dim), F), vec) + weights + (S((dim, toks), B), vec),
            in_specs=[hbm] * 9, out_specs=[vmem] * 14,
            scratch_shapes=[
                V((chunks, LANES), I), V((toks, dim), B), V((toks, dim), B), V((1, dim), F), V((1, dim), F), V((dim, ff), B), V((1, ff), F), V((ff, dim), B), pltpu.SMEM((chunks, LANES), I),
                V((2 * chunks, LANES), I), pltpu.SMEM((2 * chunks, LANES), I), V((8, LANES), F), V((8, LANES), F), V((2, TILE + 32, toks), F), V((rows, dim), F), V((rows, dim), F), V((rows, dim), F), V((rows, dim), F),
                V((8, LANES), F), V((2 * tps, 8, LANES), F), V((vocab, dim), F), V((toks, dim), F), V((8, LANES), F), V((tps, 8, LANES), F),
                DMA((PARTS,)), DMA((9,)), DMA((5,)), DMA, DMA((2,)), DMA, DMA, DMA, DMA],
            compiler_params=pltpu.CompilerParams(collective_id=0, has_side_effects=True, vmem_limit_bytes=GRANT),
        )(*stay(ids, hid, cot, ln_gamma, ln_beta, table, w_in[0], b_in, w_out[0]))
        emb_grad, w1g, b1g, w2g, part = pl.pallas_call(
            functools.partial(grad_kernel, cfg), name='grads',
            out_shape=(S((vocab, dim), F), S((dim, ff), F), S((1, ff), F), S((ff, dim), F), vec),
            in_specs=[vmem] * 14, out_specs=[hbm] * 4 + [vmem],
            scratch_shapes=[V((vocab, dim), F), V((dim, toks), F), V((dim, ff), F), V((1, ff), F), DMA((5,)), DMA((3,))],
            compiler_params=pltpu.CompilerParams(vmem_limit_bytes=GRANT),
        )(*mids)
        sums = pl.pallas_call(
            functools.partial(sum_kernel, cfg), name='sums', out_shape=vec, in_specs=[vmem] * 6, out_specs=vmem,
            scratch_shapes=[V((8, LANES), F), V((dim, toks), F), V(((stages - 2) * tps, 8, LANES), F), DMA, DMA],
            compiler_params=pltpu.CompilerParams(collective_id=1, has_side_effects=True, vmem_limit_bytes=GRANT),
        )(mids[0], mids[1], mids[4], mids[5], mids[8], part)
        vecs = pl.pallas_call(
            functools.partial(hand_kernel, cfg), name='hand', out_shape=vec, in_specs=[vmem], out_specs=vmem,
            scratch_shapes=[V((8, LANES), F), DMA, DMA],
            compiler_params=pltpu.CompilerParams(collective_id=2, has_side_effects=True, vmem_limit_bytes=4 << 20),
        )(sums)
        gam, bet, loss = pl.pallas_call(
            write_kernel, name='write', out_shape=(S((1, dim), F), S((1, dim), F), S((1,), F)), in_specs=[vmem], out_specs=[vmem] * 2 + [pl.BlockSpec(memory_space=pltpu.SMEM)],
            compiler_params=pltpu.CompilerParams(vmem_limit_bytes=4 << 20),
        )(vecs)
        return emb_grad[None], loss, gam, bet, w1g[None], b1g, w2g[None]

    rows, cols = P(lead, 'tp'), P(lead, None, 'tp')
    specs_in = (P(lead),) * 5 + (rows, cols, rows, rows)
    specs_out = (rows, P(lead), P(lead), P(lead), cols, rows, rows)
    return jax.shard_map(body, mesh=mesh, in_specs=specs_in, out_specs=specs_out, check_vma=False)
```
